64 devices in a mesh: dp: 4 (over x, y), sp: 16 (over z, core).
Axes of the slice: x: 2, y: 2, z: 8, core: 2. Of those that a mesh axis runs over, the one named last changes fastest.
The devices are a block of a 4x4x8 slice.
Arguments:
- pair_rep: float32 [1024, 256, 128], P(('dp', 'sp')), parts along dimension 0
- w_qkvg_s: bfloat16 [128, 512], replicated
- w_bias_s: bfloat16 [4, 128], replicated
- w_out_s: bfloat16 [128, 128], replicated
- w_qkvg_e: bfloat16 [128, 512], replicated
- w_bias_e: bfloat16 [4, 128], replicated
- w_out_e: bfloat16 [128, 128], replicated
- w_one: bfloat16 [128, 512], replicated
- w_two: bfloat16 [512, 128], replicated
Outputs:
- output: float32 [1024, 256, 128], P(('dp', 'sp')), parts along dimension 0
There are 4 independent parts. The reference program is written for one: setup_inputs(seed, part) draws one part's arguments, and reference() takes and returns one part's arrays. A program takes and returns all parts, laid end to end along the dimension named above; an argument that names none is the same for every part.
All inputs are finite; a program needn't handle non-finite values.
Results may differ from the reference program's by a relative error of at most 0.0105142.
Values are sent between devices in bfloat16 or wider.
A program may use at most 768 MiB of HBM per device.

```python
import jax
import jax.numpy as jnp
from jax import lax

N = 256
C_Z = 128
HEADS = 4
HEAD_DIM = C_Z // HEADS
HIDDEN = 4 * C_Z
LN_EPS = 1e-5
OUT_SCALE = (N / 16) ** 0.5


def setup_inputs(seed: int = 0, part: int = 0) -> dict:
    root_key = jax.random.key(seed)
    part_key = jax.random.fold_in(root_key, part)
    shared = jax.random.split(jax.random.fold_in(root_key, 65537), 8)
    in_scale = C_Z ** -0.5
    hid_scale = HIDDEN ** -0.5
    pair_rep = jax.random.normal(part_key, (N, N, C_Z), jnp.float32)
    w_qkvg_s = jax.random.normal(shared[0], (C_Z, 4 * C_Z), jnp.float32) * in_scale
    w_bias_s = jax.random.normal(shared[1], (HEADS, C_Z), jnp.float32) * in_scale
    w_out_s = jax.random.normal(shared[2], (C_Z, C_Z), jnp.float32) * (in_scale * OUT_SCALE)
    w_qkvg_e = jax.random.normal(shared[3], (C_Z, 4 * C_Z), jnp.float32) * in_scale
    w_bias_e = jax.random.normal(shared[4], (HEADS, C_Z), jnp.float32) * in_scale
    w_out_e = jax.random.normal(shared[5], (C_Z, C_Z), jnp.float32) * (in_scale * OUT_SCALE)
    w_one = jax.random.normal(shared[6], (C_Z, HIDDEN), jnp.float32) * in_scale
    w_two = jax.random.normal(shared[7], (HIDDEN, C_Z), jnp.float32) * hid_scale
    return {
        "pair_rep": pair_rep,
        "w_qkvg_s": w_qkvg_s.astype(jnp.bfloat16),
        "w_bias_s": w_bias_s.astype(jnp.bfloat16),
        "w_out_s": w_out_s.astype(jnp.bfloat16),
        "w_qkvg_e": w_qkvg_e.astype(jnp.bfloat16),
        "w_bias_e": w_bias_e.astype(jnp.bfloat16),
        "w_out_e": w_out_e.astype(jnp.bfloat16),
        "w_one": w_one.astype(jnp.bfloat16),
        "w_two": w_two.astype(jnp.bfloat16),
    }


def layer_norm(values):
    vals_f = values.astype(jnp.float32)
    mean_c = jnp.mean(vals_f, axis=-1, keepdims=True)
    centered = vals_f - mean_c
    variance = jnp.mean(centered * centered, axis=-1, keepdims=True)
    return (centered * lax.rsqrt(variance + LN_EPS)).astype(jnp.bfloat16)


def bias_table(pair_in, w_bias):
    def one_row(row_in):
        return jnp.dot(layer_norm(row_in), w_bias.T, preferred_element_type=jnp.float32).astype(jnp.bfloat16)
    return jnp.transpose(lax.map(one_row, pair_in), (2, 0, 1))


def row_update(row_in, bias_full, w_qkvg, w_out):
    seq_len = row_in.shape[0]
    projected = jnp.dot(layer_norm(row_in), w_qkvg, preferred_element_type=jnp.float32)
    split_shape = (seq_len, HEADS, HEAD_DIM)
    queries = projected[:, :C_Z].astype(jnp.bfloat16).reshape(split_shape).astype(jnp.float32)
    key_vecs = projected[:, C_Z:2 * C_Z].astype(jnp.bfloat16).reshape(split_shape).astype(jnp.float32)
    val_vecs = projected[:, 2 * C_Z:3 * C_Z].astype(jnp.bfloat16).reshape(split_shape).astype(jnp.float32)
    gate_vals = jax.nn.sigmoid(projected[:, 3 * C_Z:]).reshape(split_shape)
    scores = jnp.einsum('jhd,khd->hjk', queries, key_vecs) * HEAD_DIM ** -0.5 + bias_full.astype(jnp.float32)
    attn_prob = jax.nn.softmax(scores, axis=-1).astype(jnp.bfloat16).astype(jnp.float32)
    attn_out = jnp.einsum('hjk,khd->jhd', attn_prob, val_vecs)
    gated_out = (attn_out * gate_vals).astype(jnp.bfloat16).reshape(seq_len, C_Z)
    return jnp.dot(gated_out, w_out, preferred_element_type=jnp.float32)


def tri_attention(pair_in, w_qkvg, w_bias, w_out):
    bias_full = bias_table(pair_in, w_bias)

    def one_row(row_in):
        return row_update(row_in, bias_full, w_qkvg, w_out)
    return lax.map(one_row, pair_in)


def reference(pair_rep, w_qkvg_s, w_bias_s, w_out_s, w_qkvg_e, w_bias_e, w_out_e, w_one, w_two):
    pair_one = pair_rep + tri_attention(pair_rep, w_qkvg_s, w_bias_s, w_out_s)
    pair_trans = jnp.swapaxes(pair_one.astype(jnp.bfloat16), 0, 1)
    end_upd = tri_attention(pair_trans, w_qkvg_e, w_bias_e, w_out_e)

    def finish_row(row_pair):
        trans_row, upd_row = row_pair
        pair_two = trans_row.astype(jnp.float32) + upd_row
        hidden = jax.nn.relu(jnp.dot(layer_norm(pair_two), w_one, preferred_element_type=jnp.float32))
        trans_out = jnp.dot(hidden.astype(jnp.bfloat16), w_two, preferred_element_type=jnp.float32)
        return (upd_row + trans_out).astype(jnp.bfloat16)

    delta_trans = lax.map(finish_row, (pair_trans, end_upd))
    return pair_one + jnp.swapaxes(delta_trans, 0, 1).astype(jnp.float32)
```

```python
import functools

import jax
import jax.numpy as jnp
from jax import lax
from jax.experimental import pallas as pl
from jax.experimental.pallas import tpu as pltpu
from jax.sharding import PartitionSpec as P

LN_EPS = 1e-5
F32, BF16 = jnp.float32, jnp.bfloat16
MESH = pl.DeviceIdType.MESH
AXIS = "sp"
CORES = 2
ROW_UNROLL = 2
COL_GROUP = 4
COL_UNROLL = 2


def norm(vals):
    mean_c = jnp.mean(vals, axis=-1, keepdims=True)
    centered = vals - mean_c
    variance = jnp.mean(centered * centered, axis=-1, keepdims=True)
    return (centered * lax.rsqrt(variance + LN_EPS)).astype(BF16)


def mm(a, b, ca=1, cb=0):
    return lax.dot_general(a, b, (((ca,), (cb,)), ((), ())), preferred_element_type=F32)


def sigmoid(x):
    return 1.0 / (1.0 + jnp.exp(-x))


def kernel(n, rows, seq, heads, z_ref, wp_s, wb_s, wo_s, wp_e, wb_e, wo_e, w1, w2,
           z1_ref, drecv,
           u_s, q_s, kt_s, v_s, g_s, bacc, brecv, bias_f, hsend, ht, erecv, bias_e, dsend, wt_e,
           b_ss, b_rs, bf_ss, e_ss, e_rs, ef_ss, h_ss, h_rs, d_ss, d_rs):
    chan = wo_s.shape[0]
    hd = chan // heads
    scale = hd ** -0.5
    chips = n // CORES
    me = lax.axis_index(AXIS)
    chip, core = me // CORES, lax.rem(me, CORES)
    partner = chip * CORES + (CORES - 1 - core)
    hrows = heads * rows

    def remote(src, dst, ss, rs, dev):
        return pltpu.make_async_remote_copy(src_ref=src, dst_ref=dst, send_sem=ss, recv_sem=rs,
                                            device_id={AXIS: dev}, device_id_type=MESH)

    barrier = pltpu.get_barrier_semaphore()
    for off in range(1, n):
        pl.semaphore_signal(barrier, 1, device_id={AXIS: lax.rem(me + off, n)}, device_id_type=MESH)

    def spread(wb):
        wide = wb[...].astype(F32)
        return jnp.concatenate([jnp.broadcast_to(wide[h:h + 1], (rows, chan)) for h in range(heads)], axis=0)

    row_of = lax.rem(lax.broadcasted_iota(jnp.int32, (hrows, chan), 0), rows)
    lane_head = lax.broadcasted_iota(jnp.int32, (1, chan), 1) // hd

    def pair_bias(get_row, put_row, wb, out):
        wide = spread(wb)
        bacc[...] = jnp.zeros_like(bacc)

        def step(i, carry):
            total = None
            for t in range(2):
                r = 2 * i + t
                u = norm(get_row(r))
                if put_row is not None:
                    put_row(r, u)
                picked = jnp.where(row_of == r, wide, 0.0).astype(BF16)
                part = mm(picked, u, 1, 1)
                total = part if total is None else total + part
            bacc[...] += total
            return carry

        lax.fori_loop(0, rows // 2, step, 0)
        out[me] = bacc[...].astype(BF16)

    def bias_copy(buf, ss, rs, dev):
        return remote(buf.at[me], buf.at[me], ss.at[dev], rs.at[me], dev)

    def bias_send(buf, ss, rs):
        bias_copy(buf, ss, rs, partner).start()
        for dist in range(1, chips):
            off = (dist + 1) // 2 if dist % 2 else chips - dist // 2
            bias_copy(buf, ss, rs, lax.rem(chip + off, chips) * CORES + core).start()

    def bias_wait(buf, ss, rs, src):
        remote(buf.at[src], buf.at[src], ss.at[src], rs.at[src], partner).wait_recv()

    def forward(buf, ss, rs, c):
        src = c * CORES + core
        return remote(buf.at[src], buf.at[src], ss.at[c], rs.at[src], partner)

    def bias_drain(buf, ss, rs, fss):
        bias_copy(buf, ss, rs, partner).wait_send()
        for dist in range(1, chips):
            c = lax.rem(chip + dist, chips)
            bias_copy(buf, ss, rs, c * CORES + core).wait_send()
            forward(buf, fss, rs, c).wait_send()

    def put_u(r, u):
        u_s[r] = u

    pair_bias(lambda r: z_ref[r], put_u, wb_s, brecv)
    pl.semaphore_wait(barrier, n - 1)
    bias_send(brecv, b_ss, b_rs)

    wk_t = wp_s[:, chan:2 * chan].astype(F32).T.astype(BF16)

    def project(i, carry):
        for t in range(2):
            r = 2 * i + t
            u = u_s[r]
            pr = mm(u, wp_s[...])
            q_s[r] = pr[:, :chan].astype(BF16)
            kt_s[r] = mm(wk_t, u, 1, 1).astype(BF16)
            v_s[r] = pr[:, 2 * chan:3 * chan].astype(BF16)
            g_s[r] = sigmoid(pr[:, 3 * chan:])
        return carry

    lax.fori_loop(0, rows // 2, project, 0)

    blk = CORES * rows
    nq = 2 * blk

    def chips_of(p):
        return lax.rem(chip + chips - p, chips), lax.rem(chip + p + 1, chips)

    def fetch_bias(p):
        for c in chips_of(p):
            @pl.when(c != chip)
            def _():
                bias_wait(brecv, b_ss, b_rs, c * CORES + core)
                forward(brecv, bf_ss, b_rs, c).start()

    fetch_bias(0)

    def start_pair(p, carry):
        ca, cb = chips_of(p)
        for c in (ca, cb):
            bias_wait(brecv, b_ss, b_rs, c * CORES + (CORES - 1 - core))
        devs = [c * CORES + s for c in (ca, cb) for s in range(CORES)]
        for h in range(heads):
            for k, dev in enumerate(devs):
                bias_f[h * nq + k * rows:h * nq + (k + 1) * rows, :] = brecv[dev, h * rows:(h + 1) * rows, :].astype(F32)
        cols = [pl.ds(pl.multiple_of(c * blk, blk), blk) for c in (ca, cb)]

        def attend(i, carry):
            rs = [ROW_UNROLL * i + t for t in range(ROW_UNROLL)]
            qs = [jnp.concatenate([q_s[r, cs, :] for cs in cols], axis=0) for r in rs]
            qm = [jnp.concatenate([jnp.where(lane_head == h, q, jnp.zeros_like(q)) for h in range(heads)], axis=0) for q in qs]
            sc = [mm(a, kt_s[r]) * scale + bias_f[...] for a, r in zip(qm, rs)]
            pe = [jnp.exp(s - jnp.max(s, axis=-1, keepdims=True)) for s in sc]
            ls = [1.0 / jnp.sum(e, axis=-1, keepdims=True) for e in pe]
            os = [mm(e.astype(BF16), v_s[r]) * l for e, r, l in zip(pe, rs, ls)]
            upds = []
            for r, o in zip(rs, os):
                mix = sum(jnp.where(lane_head == h, o[h * nq:(h + 1) * nq], 0.0) for h in range(heads))
                gate = jnp.concatenate([g_s[r, cs, :] for cs in cols], axis=0)
                upds.append(mm((mix * gate).astype(BF16), wo_s[...]))
            for r, upd in zip(rs, upds):
                for k, c in enumerate((ca, cb)):
                    z1_ref[pl.ds(pl.multiple_of(r * seq + c * blk, blk), blk), :] = (
                        z_ref[r, cols[k], :] + upd[k * blk:(k + 1) * blk])
            return carry

        half = rows // ROW_UNROLL // 2
        lax.fori_loop(0, half, attend, 0)

        @pl.when(p + 1 < chips // 2)
        def _():
            fetch_bias(p + 1)

        lax.fori_loop(half, 2 * half, attend, 0)

        for dev in devs:
            for j in range(rows):
                col = dev * rows + j
                hsend[col] = z1_ref[pl.ds(col, rows, stride=seq), :].astype(BF16)
        for dev in devs:
            @pl.when(dev != me)
            def _():
                h_copy(dev).start()

            @pl.when(dev == me)
            def _():
                ht[:, pl.ds(pl.multiple_of(me * rows, rows), rows), :] = hsend[pl.ds(pl.multiple_of(me * rows, rows), rows)]
        return carry

    def h_copy(dev):
        return remote(hsend.at[pl.ds(dev * rows, rows)], ht.at[:, pl.ds(pl.multiple_of(me * rows, rows), rows), :],
                      h_ss.at[dev], h_rs.at[me], dev)

    def h_wait(src):
        remote(hsend.at[pl.ds(src * rows, rows)], ht.at[:, pl.ds(pl.multiple_of(src * rows, rows), rows), :],
               h_ss.at[src], h_rs.at[src], src).wait_recv()

    lax.fori_loop(0, chips // 2, start_pair, 0)

    pair_bias(lambda r: z1_ref[pl.ds(pl.multiple_of(r * seq, seq), seq), :].astype(BF16).astype(F32), None, wb_e, erecv)
    bias_send(erecv, e_ss, e_rs)
    wide = wp_e[...].astype(F32)
    wt_e[...] = jnp.concatenate([wide[:, :chan], wide[:, 2 * chan:]], axis=1).T.astype(BF16)

    for dist in range(1, chips):
        off = (dist + 1) // 2 if dist % 2 else chips - dist // 2
        c = lax.rem(chip + off, chips)
        bias_wait(erecv, e_ss, e_rs, c * CORES + core)
        forward(erecv, ef_ss, e_rs, c).start()
    for c in range(chips):
        bias_wait(erecv, e_ss, e_rs, c * CORES + (CORES - 1 - core))

    def widen(dev, carry):
        for h in range(heads):
            bias_e[h, pl.ds(pl.multiple_of(dev * rows, rows), rows), :] = erecv[dev, h * rows:(h + 1) * rows, :].astype(F32)
        return carry

    lax.fori_loop(0, n, widen, 0)
    for off in range(1, n):
        h_wait(lax.rem(me + off, n))

    def d_copy(dev, grp):
        src = dsend.at[pl.ds(grp * COL_GROUP, COL_GROUP), pl.ds(pl.multiple_of(dev * rows, rows), rows), :]
        dst = drecv.at[pl.ds(me * rows + grp * COL_GROUP, COL_GROUP)]
        return remote(src, dst, d_ss.at[dev, grp], d_rs.at[me, grp], dev)

    def end_cols(i, carry):
        js = [COL_UNROLL * i + t for t in range(COL_UNROLL)]
        hs = [ht[j] for j in js]
        us = [norm(h.astype(F32)) for h in hs]
        keys = [mm(u, wp_e[:, chan:2 * chan]).astype(BF16) for u in us]
        trs = [mm(wt_e[...], u, 1, 1) for u in us]
        es = []
        for key, tr in zip(keys, trs):
            qt = tr[:chan].astype(BF16)
            vt = tr[chan:2 * chan].astype(BF16)
            gt = sigmoid(tr[2 * chan:])
            parts = []
            for h in range(heads):
                pieces = [jnp.zeros((hd, seq), BF16)] * heads
                pieces[h] = qt[h * hd:(h + 1) * hd]
                s = mm(key, jnp.concatenate(pieces, axis=0)) * scale + bias_e[h]
                e = jnp.exp(s - jnp.max(s, axis=0, keepdims=True))
                l = 1.0 / jnp.sum(e, axis=0, keepdims=True)
                parts.append(mm(vt[h * hd:(h + 1) * hd], e.astype(BF16)) * l)
            og = (jnp.concatenate(parts, axis=0) * gt).astype(BF16)
            es.append(mm(og, wo_e[...], 0, 0))
        z2 = [h.astype(F32) + e for h, e in zip(hs, es)]
        hid = [jnp.maximum(mm(norm(z), w1[...]), 0.0).astype(BF16) for z in z2]
        ts = [mm(x, w2[...]) for x in hid]
        for j, e, t in zip(js, es, ts):
            dsend[j] = (e + t).astype(BF16)
        return carry

    def end_group(grp, carry):
        lax.fori_loop(grp * (COL_GROUP // COL_UNROLL), (grp + 1) * (COL_GROUP // COL_UNROLL), end_cols, 0)
        for off in range(1, n):
            d_copy(lax.rem(me + off, n), grp).start()
        drecv[pl.ds(me * rows + grp * COL_GROUP, COL_GROUP)] = (
            dsend[pl.ds(grp * COL_GROUP, COL_GROUP), pl.ds(pl.multiple_of(me * rows, rows), rows), :])
        return carry

    lax.fori_loop(0, rows // COL_GROUP, end_group, 0)

    bias_drain(brecv, b_ss, b_rs, bf_ss)
    bias_drain(erecv, e_ss, e_rs, ef_ss)
    for off in range(1, n):
        dev = lax.rem(me + off, n)
        h_copy(dev).wait_send()
        for grp in range(rows // COL_GROUP):
            d_copy(dev, grp).wait_send()
            src = dsend.at[pl.ds(grp * COL_GROUP, COL_GROUP), pl.ds(pl.multiple_of(dev * rows, rows), rows), :]
            dst = drecv.at[pl.ds(dev * rows + grp * COL_GROUP, COL_GROUP)]
            remote(src, dst, d_ss.at[dev, grp], d_rs.at[dev, grp], dev).wait_recv()


def solution(mesh):
    row_spec = P(('dp', AXIS), None, None)
    n = mesh.shape[AXIS]

    def local_fn(z, wp_s, wb_s, wo_s, wp_e, wb_e, wo_e, w1, w2):
        rows, seq, chan = z.shape
        heads = wb_s.shape[0]
        hrows = heads * rows
        nq = 2 * CORES * rows
        dma = pltpu.SemaphoreType.DMA
        groups = rows // COL_GROUP
        vmem = pl.BlockSpec(memory_space=pltpu.VMEM)
        z1, delta = pl.pallas_call(
            functools.partial(kernel, n, rows, seq, heads),
            out_shape=(jax.ShapeDtypeStruct((rows * seq, chan), F32), jax.ShapeDtypeStruct((seq, rows, chan), BF16)),
            in_specs=[vmem] * 9,
            out_specs=(vmem, vmem),
            scratch_shapes=[
                pltpu.VMEM((rows, seq, chan), BF16),
                pltpu.VMEM((rows, seq, chan), BF16),
                pltpu.VMEM((rows, chan, seq), BF16),
                pltpu.VMEM((rows, seq, chan), BF16),
                pltpu.VMEM((rows, seq, chan), F32),
                pltpu.VMEM((hrows, seq), F32),
                pltpu.VMEM((n, hrows, seq), BF16),
                pltpu.VMEM((heads * nq, seq), F32),
                pltpu.VMEM((seq, rows, chan), BF16),
                pltpu.VMEM((rows, seq, chan), BF16),
                pltpu.VMEM((n, hrows, seq), BF16),
                pltpu.VMEM((heads, seq, seq), F32),
                pltpu.VMEM((rows, seq, chan), BF16),
                pltpu.VMEM((3 * chan, chan), BF16),
                dma((n,)), dma((n,)), dma((n,)), dma((n,)), dma((n,)), dma((n,)),
                dma((n,)), dma((n,)), dma((n, groups)), dma((n, groups)),
            ],
            compiler_params=pltpu.CompilerParams(collective_id=0, has_side_effects=True),
        )(z, wp_s, wb_s, wo_s, wp_e, wb_e, wo_e, w1, w2)
        return z1.reshape(rows, seq, chan) + jnp.swapaxes(delta, 0, 1).astype(F32)

    return jax.shard_map(local_fn, mesh=mesh, in_specs=(row_spec,) + (P(),) * 8, out_specs=row_spec, check_vma=False)
```

```python
import functools

import jax
import jax.numpy as jnp
from jax import lax
from jax.experimental import pallas as pl
from jax.experimental.pallas import tpu as pltpu
from jax.sharding import PartitionSpec as P

LN_EPS = 1e-5
F32, BF16 = jnp.float32, jnp.bfloat16
MESH = pl.DeviceIdType.MESH
AXIS = "sp"
CORES = 2
HALVES = 2
GROUPS = 2
ROW_UNROLL = 8
COL_UNROLL = 2
LN_UNROLL = 4
PAD = 8


def norm(vals):
    mean_c = jnp.mean(vals, axis=-1, keepdims=True)
    centered = vals - mean_c
    variance = jnp.mean(centered * centered, axis=-1, keepdims=True)
    return (centered * lax.rsqrt(variance + LN_EPS)).astype(BF16)


def mm(a, b, ca=1, cb=0):
    return lax.dot_general(a, b, (((ca,), (cb,)), ((), ())), preferred_element_type=F32)


def sigmoid(x):
    return 1.0 / (1.0 + jnp.exp(-x))


def kernel(n, rows, seq, heads, z_hbm, wps_h, wbs_h, wos_h, wpe_h, wbe_h, woe_h, w1_h, w2_h,
           z1_ref, drecv,
           z_ref, wp_s, wb_s, wo_s, wp_e, wb_e, wo_e, w1, w2,
           u_s, q_s, kt_s, v_s, g_s, bacc, brecv, bias_all, bias_f, zb, hsend, ht, erecv, bias_e, stage, dsend, wk_s, wk_e,
           z_sem, w_sem, b_ss, b_rs, bf_ss, e_ss, e_rs, ef_ss, h_ss, h_rs, d_ss, d_rs):
    chan = wo_s.shape[0]
    hd = chan // heads
    scale = hd ** -0.5
    chips = n // CORES
    part = rows // HALVES
    me = lax.axis_index(AXIS)
    chip, core = me // CORES, lax.rem(me, CORES)
    other = CORES - 1 - core
    partner = chip * CORES + other
    hrows = heads * rows

    def remote(src, dst, ss, rs, dev):
        return pltpu.make_async_remote_copy(src_ref=src, dst_ref=dst, send_sem=ss, recv_sem=rs,
                                            device_id={AXIS: dev}, device_id_type=MESH)

    def aligned(i, k):
        return pl.multiple_of(i, k)

    barrier = pltpu.get_barrier_semaphore()
    for off in range(1, n):
        pl.semaphore_signal(barrier, 1, device_id={AXIS: lax.rem(me + off, n)}, device_id_type=MESH)

    def z_load(i):
        sl = pl.ds(i * LN_UNROLL, LN_UNROLL)
        return pltpu.make_async_copy(z_hbm.at[sl], z_ref.at[sl], z_sem.at[i])

    w_loads = [pltpu.make_async_copy(src, dst, w_sem.at[i]) for i, (src, dst) in enumerate(
        [(wbs_h, wb_s), (wps_h, wp_s), (wos_h, wo_s), (wbe_h, wb_e), (wpe_h, wp_e), (woe_h, wo_e), (w1_h, w1), (w2_h, w2)])]
    w_loads[0].start()
    for i in range(rows // LN_UNROLL):
        z_load(i).start()
    for cp in w_loads[1:]:
        cp.start()

    row_of = lax.rem(lax.broadcasted_iota(jnp.int32, (hrows, chan), 0), rows)
    lane_head = lax.broadcasted_iota(jnp.int32, (1, chan), 1) // hd

    def pair_bias(ready, get_row, put_row, wb, out):
        wide = wb[...].astype(F32)
        wide = jnp.concatenate([jnp.broadcast_to(wide[h:h + 1], (rows, chan)) for h in range(heads)], axis=0)
        bacc[...] = jnp.zeros_like(bacc)

        def step(i, carry):
            ready(i)
            rs = [LN_UNROLL * i + t for t in range(LN_UNROLL)]
            us = [norm(get_row(r)) for r in rs]
            total = sum(mm(jnp.where(row_of == r, wide, 0.0).astype(BF16), u, 1, 1) for r, u in zip(rs, us))
            if put_row is not None:
                for r, u in zip(rs, us):
                    put_row(r, u)
            bacc[...] += total
            return carry

        lax.fori_loop(0, rows // LN_UNROLL, step, 0)
        out[me] = bacc[...].astype(BF16)

    def bias_copy(buf, ss, rs, dev):
        return remote(buf.at[me], buf.at[me], ss.at[dev], rs.at[me], dev)

    def by_distance(dist):
        return lax.rem(chip + ((dist + 1) // 2 if dist % 2 else chips - dist // 2), chips)

    def bias_send(buf, ss, rs):
        bias_copy(buf, ss, rs, partner).start()
        for dist in range(1, chips):
            bias_copy(buf, ss, rs, by_distance(dist) * CORES + core).start()

    def bias_wait(buf, ss, rs, src):
        remote(buf.at[src], buf.at[src], ss.at[src], rs.at[src], partner).wait_recv()

    def forward(buf, ss, rs, c):
        src = c * CORES + core
        return remote(buf.at[src], buf.at[src], ss.at[c], rs.at[src], partner)

    def bias_drain(buf, ss, rs, fss):
        bias_copy(buf, ss, rs, partner).wait_send()
        for dist in range(1, chips):
            c = by_distance(dist)
            bias_copy(buf, ss, rs, c * CORES + core).wait_send()
            forward(buf, fss, rs, c).wait_send()

    def put_u(r, u):
        u_s[r] = u

    w_loads[0].wait()
    with jax.named_scope("bias_rows"):
        pair_bias(lambda i: z_load(i).wait(), lambda r: z_ref[r], put_u, wb_s, brecv)
    with jax.named_scope("barrier"):
        pl.semaphore_wait(barrier, n - 1)
    bias_send(brecv, b_ss, b_rs)
    for cp in w_loads[1:]:
        cp.wait()

    wk_s[...] = wp_s[:, chan:2 * chan].astype(F32).T.astype(BF16)
    wk_e[...] = wp_e[:, chan:2 * chan].astype(F32).T.astype(BF16)

    def by_part(x):
        return jnp.concatenate([x[d * rows + hf * part:d * rows + (hf + 1) * part] for hf in range(HALVES) for d in range(n)], axis=0)

    def project(i, carry):
        for t in range(2):
            r = 2 * i + t
            u = u_s[r]
            pr = mm(u, wp_s[...])
            q_s[r] = by_part(pr[:, :chan]).astype(BF16)
            kt_s[r] = mm(wk_s[...], u, 1, 1).astype(BF16)
            v_s[r] = pr[:, 2 * chan:3 * chan].astype(BF16)
            g_s[r] = by_part(sigmoid(pr[:, 3 * chan:]))
        return carry

    with jax.named_scope("project"):
        lax.fori_loop(0, rows // 2, project, 0)

    gchips = chips // GROUPS
    nq = gchips * CORES * part

    def chips_of(g):
        offs = (chips - 2 * g, 1 + 2 * g, chips - 1 - 2 * g, 2 + 2 * g)
        return [lax.rem(chip + off, chips) for off in offs]

    def fetch_bias(g):
        for c in chips_of(g):
            @pl.when(c != chip)
            def _():
                bias_wait(brecv, b_ss, b_rs, c * CORES + core)
                forward(brecv, bf_ss, b_rs, c).start()

    def attention(qs, kts, vs, biases, gates, wo):
        nrow = qs[0].shape[0]
        qm = [jnp.concatenate([jnp.where(lane_head == h, q, jnp.zeros_like(q)) for h in range(heads)], axis=0) for q in qs]
        sc = [mm(a, kt) * scale + b[...] for a, kt, b in zip(qm, kts, biases)]
        pe = [jnp.exp(s - jnp.max(s, axis=-1, keepdims=True)) for s in sc]
        ls = [1.0 / jnp.sum(e, axis=-1, keepdims=True) for e in pe]
        os = [mm(e.astype(BF16), v) * l for e, v, l in zip(pe, vs, ls)]
        upds = []
        for o, gate in zip(os, gates):
            mix = sum(jnp.where(lane_head == h, o[h * nrow:(h + 1) * nrow], 0.0) for h in range(heads))
            upds.append(mm((mix * gate).astype(BF16), wo[...]))
        return upds

    def h_copy(dev, hf):
        return remote(hsend.at[pl.ds(dev * rows + hf * part, part)],
                      ht.at[pl.ds(hf * part, part), pl.ds(aligned(me * rows, rows), rows), :],
                      h_ss.at[dev, hf], h_rs.at[me, hf], dev)

    def h_wait(src, hf):
        remote(hsend.at[pl.ds(src * rows + hf * part, part)],
               ht.at[pl.ds(hf * part, part), pl.ds(aligned(src * rows, rows), rows), :],
               h_ss.at[src, hf], h_rs.at[src, hf], src).wait_recv()

    with jax.named_scope("fetch_first"):
        fetch_bias(0)

    def start_block(b, carry):
        hf, g = b // GROUPS, lax.rem(b, GROUPS)
        cs = chips_of(g)
        devs = [c * CORES + s for c in cs for s in range(CORES)]

        @pl.when(hf == 0)
        def _():
            with jax.named_scope("wait_block"):
                for c in cs:
                    bias_wait_other(c)
            for dev in devs:
                bias_all[dev] = brecv[dev].astype(F32)

        for h in range(heads):
            for k, dev in enumerate(devs):
                bias_f[h * nq + k * part:h * nq + (k + 1) * part, :] = bias_all[dev, pl.ds(aligned(h * rows + hf * part, part), part), :]
        wide = CORES * part
        qcols = [pl.ds(aligned((hf * chips + c) * wide, wide), wide) for c in cs]
        zcols = [aligned(dev * rows + hf * part, part) for dev in devs]

        def attend(i, carry):
            rs = [ROW_UNROLL * i + t for t in range(ROW_UNROLL)]
            qs = [jnp.concatenate([q_s[r, sl, :] for sl in qcols], axis=0) for r in rs]
            gates = [jnp.concatenate([g_s[r, sl, :] for sl in qcols], axis=0) for r in rs]
            upds = attention(qs, [kt_s[r] for r in rs], [v_s[r] for r in rs], [bias_f] * len(rs), gates, wo_s)
            for r, upd in zip(rs, upds):
                z1 = jnp.concatenate([z_ref[r, pl.ds(zc, part), :] for zc in zcols], axis=0) + upd
                for k, zc in enumerate(zcols):
                    z1_ref[pl.ds(aligned(r * seq + zc, part), part), :] = z1[k * part:(k + 1) * part]
                zb[pl.ds(aligned(r * (nq + PAD), PAD), nq), :] = z1
            return carry

        half = rows // ROW_UNROLL // 2
        with jax.named_scope("attend_a"):
            lax.fori_loop(0, half, attend, 0)
        with jax.named_scope("fetch_next"):
            @pl.when(b == 0)
            def _():
                fetch_bias(1)
        with jax.named_scope("attend_b"):
            lax.fori_loop(half, 2 * half, attend, 0)

        for k, dev in enumerate(devs):
            for j in range(part):
                hsend[dev * rows + hf * part + j] = zb[pl.ds(k * part + j, rows, stride=nq + PAD), :].astype(BF16)
        for dev in devs:
            @pl.when(jnp.logical_and(dev != me, hf == 0))
            def _():
                h_copy(dev, hf).start()
        return carry

    def bias_wait_other(c):
        bias_wait(brecv, b_ss, b_rs, c * CORES + other)

    lax.fori_loop(0, HALVES * GROUPS, start_block, 0)

    with jax.named_scope("bias_cols"):
        pair_bias(lambda i: None, lambda r: z1_ref[pl.ds(aligned(r * seq, seq), seq), :].astype(BF16).astype(F32), None, wb_e, erecv)
    bias_send(erecv, e_ss, e_rs)
    for hf in range(1, HALVES):
        for off in range(1, n):
            h_copy(lax.rem(me + off, n), hf).start()
    ht[:, pl.ds(aligned(me * rows, rows), rows), :] = hsend[pl.ds(aligned(me * rows, rows), rows)]

    with jax.named_scope("wait_cols"):
        for dist in range(1, chips):
            c = by_distance(dist)
            bias_wait(erecv, e_ss, e_rs, c * CORES + core)
            forward(erecv, ef_ss, e_rs, c).start()
        for c in range(chips):
            bias_wait(erecv, e_ss, e_rs, c * CORES + other)

    def widen(h, carry):
        tall = jnp.concatenate([erecv[dev, pl.ds(aligned(h * rows, rows), rows), :] for dev in range(n)], axis=0)
        bias_e[pl.ds(aligned(h * seq, seq), seq), :] = tall.astype(F32).T
        return carry

    with jax.named_scope("widen"):
        lax.fori_loop(0, heads, widen, 0)

    def d_copy(dev, hf):
        return remote(dsend.at[hf, pl.ds(dev * rows, rows)], drecv.at[:, me, hf], d_ss.at[dev, hf], d_rs.at[me, hf], dev)

    def end_cols(hf, i, carry):
        js = [COL_UNROLL * i + t for t in range(COL_UNROLL)]
        hs = [ht[hf * part + j] for j in js]
        us = [norm(h.astype(F32)) for h in hs]
        prs = [mm(u, wp_e[...]) for u in us]
        kts = [mm(wk_e[...], u, 1, 1).astype(BF16) for u in us]
        es = attention([p[:, :chan].astype(BF16) for p in prs], kts, [p[:, 2 * chan:3 * chan].astype(BF16) for p in prs],
                       [bias_e] * len(js), [sigmoid(p[:, 3 * chan:]) for p in prs], wo_e)
        z2 = [h.astype(F32) + e for h, e in zip(hs, es)]
        hid = [jnp.maximum(mm(norm(z), w1[...]), 0.0).astype(BF16) for z in z2]
        ts = [mm(x, w2[...]) for x in hid]
        for j, e, t in zip(js, es, ts):
            stage[pl.ds(aligned(j * (seq + PAD), PAD), seq), :] = e + t
        return carry

    for hf in range(HALVES):
        with jax.named_scope("wait_h"):
            for off in range(1, n):
                h_wait(lax.rem(me + off, n), hf)
        with jax.named_scope("end_cols"):
            lax.fori_loop(0, part // COL_UNROLL, functools.partial(end_cols, hf), 0)

        def pack(dev, carry):
            for t in range(rows):
                i = dev * rows + t
                dsend[hf, i] = stage[pl.ds(i, part, stride=seq + PAD), :].astype(BF16)
            return carry

        with jax.named_scope("pack"):
            lax.fori_loop(0, n, pack, 0)
        for off in range(1, n):
            d_copy(lax.rem(me + off, n), hf).start()
        drecv[:, me, hf] = dsend[hf, pl.ds(me * rows, rows)]

    with jax.named_scope("drain"):
        bias_drain(brecv, b_ss, b_rs, bf_ss)
        bias_drain(erecv, e_ss, e_rs, ef_ss)
        for off in range(1, n):
            dev = lax.rem(me + off, n)
            for hf in range(HALVES):
                h_copy(dev, hf).wait_send()
                d_copy(dev, hf).wait_send()
                remote(dsend.at[hf, pl.ds(dev * rows, rows)], drecv.at[:, dev, hf], d_ss.at[dev, hf], d_rs.at[dev, hf], dev).wait_recv()


def solution(mesh):
    row_spec = P(('dp', AXIS), None, None)
    n = mesh.shape[AXIS]

    def local_fn(z, *weights):
        rows, seq, chan = z.shape
        heads = weights[1].shape[0]
        hrows = heads * rows
        part = rows // HALVES
        nq = n // GROUPS * part
        dma = pltpu.SemaphoreType.DMA
        vmem = pl.BlockSpec(memory_space=pltpu.VMEM)
        z1, delta = pl.pallas_call(
            functools.partial(kernel, n, rows, seq, heads),
            out_shape=(jax.ShapeDtypeStruct((rows * seq, chan), F32), jax.ShapeDtypeStruct((rows, n, HALVES, part, chan), BF16)),
            in_specs=[pl.BlockSpec(memory_space=pltpu.HBM)] * 9,
            out_specs=(vmem, vmem),
            scratch_shapes=[pltpu.VMEM(z.shape, z.dtype)] + [pltpu.VMEM(w.shape, w.dtype) for w in weights] + [
                pltpu.VMEM((rows, seq, chan), BF16),
                pltpu.VMEM((rows, seq, chan), BF16),
                pltpu.VMEM((rows, chan, seq), BF16),
                pltpu.VMEM((rows, seq, chan), BF16),
                pltpu.VMEM((rows, seq, chan), F32),
                pltpu.VMEM((hrows, seq), F32),
                pltpu.VMEM((n, hrows, seq), BF16),
                pltpu.VMEM((n, hrows, seq), F32),
                pltpu.VMEM((heads * nq, seq), F32),
                pltpu.VMEM((rows * (nq + PAD), chan), F32),
                pltpu.VMEM((seq, rows, chan), BF16),
                pltpu.VMEM((rows, seq, chan), BF16),
                pltpu.VMEM((n, hrows, seq), BF16),
                pltpu.VMEM((heads * seq, seq), F32),
                pltpu.VMEM((part * (seq + PAD), chan), F32),
                pltpu.VMEM((HALVES, seq, part, chan), BF16),
                pltpu.VMEM((chan, chan), BF16),
                pltpu.VMEM((chan, chan), BF16),
                dma((rows // LN_UNROLL,)), dma((len(weights),)),
                dma((n,)), dma((n,)), dma((n,)), dma((n,)), dma((n,)), dma((n,)),
                dma((n, HALVES)), dma((n, HALVES)), dma((n, HALVES)), dma((n, HALVES)),
            ],
            compiler_params=pltpu.CompilerParams(collective_id=0, has_side_effects=True, vmem_limit_bytes=40 * 2 ** 20),
        )(*[pltpu.with_memory_space_constraint(a, pltpu.HBM) for a in (z,) + weights])
        return z1.reshape(rows, seq, chan) + delta.reshape(rows, seq, chan).astype(F32)

    return jax.shard_map(local_fn, mesh=mesh, in_specs=(row_spec,) + (P(),) * 8, out_specs=row_spec, check_vma=False)
```

```python
import functools

import jax
import jax.numpy as jnp
from jax import lax
from jax.experimental import pallas as pl
from jax.experimental.pallas import tpu as pltpu
from jax.sharding import PartitionSpec as P

LN_EPS = 1e-5
F32, BF16 = jnp.float32, jnp.bfloat16
MESH = pl.DeviceIdType.MESH
AXIS = "sp"
CORES = 2
HALVES = 2
COL_GROUP = 4
HOLD_FROM = 2
ROW_UNROLL = 8
COL_UNROLL = 2
LN_UNROLL = 4
PAD = 8


def norm(vals):
    mean_c = jnp.mean(vals, axis=-1, keepdims=True)
    centered = vals - mean_c
    variance = jnp.mean(centered * centered, axis=-1, keepdims=True)
    return (centered * lax.rsqrt(variance + LN_EPS)).astype(BF16)


def mm(a, b, ca=1, cb=0):
    return lax.dot_general(a, b, (((ca,), (cb,)), ((), ())), preferred_element_type=F32)


def sigmoid(x):
    return 1.0 / (1.0 + jnp.exp(-x))


def kernel(n, rows, seq, heads, z_hbm, wps_h, wbs_h, wos_h, wpe_h, wbe_h, woe_h, w1_h, w2_h,
           z1_ref,
           z_ref, wp_s, wb_s, wo_s, wp_e, wb_e, wo_e, w1, w2,
           u_s, q_s, kt_s, v_s, g_s, bacc, brecv, bias_f, zb, hsend, ht, erecv, bias_e, dsend, drecv, tmp,
           z_sem, w_sem, b_ss, b_rs, e_ss, e_rs, h_ss, h_rs, d_ss, d_rs):
    chan = wo_s.shape[0]
    hd = chan // heads
    scale = hd ** -0.5
    chips = n // CORES
    part = rows // HALVES
    me = lax.axis_index(AXIS)
    chip, core = me // CORES, lax.rem(me, CORES)
    other = CORES - 1 - core
    partner = chip * CORES + other
    hrows = heads * rows

    def remote(src, dst, ss, rs, dev):
        return pltpu.make_async_remote_copy(src_ref=src, dst_ref=dst, send_sem=ss, recv_sem=rs,
                                            device_id={AXIS: dev}, device_id_type=MESH)

    def aligned(i, k):
        return pl.multiple_of(i, k)

    barrier = pltpu.get_barrier_semaphore()
    for off in range(1, n):
        pl.semaphore_signal(barrier, 1, device_id={AXIS: lax.rem(me + off, n)}, device_id_type=MESH)

    def z_load(i):
        sl = pl.ds(i * LN_UNROLL, LN_UNROLL)
        return pltpu.make_async_copy(z_hbm.at[sl], z_ref.at[sl], z_sem.at[i])

    w_loads = [pltpu.make_async_copy(src, dst, w_sem.at[i]) for i, (src, dst) in enumerate(
        [(wbs_h, wb_s), (wps_h, wp_s), (wos_h, wo_s), (wbe_h, wb_e), (wpe_h, wp_e), (woe_h, wo_e), (w1_h, w1), (w2_h, w2)])]
    w_loads[0].start()
    for i in range(rows // LN_UNROLL):
        z_load(i).start()
    for cp in w_loads[1:]:
        cp.start()

    row_of = lax.rem(lax.broadcasted_iota(jnp.int32, (hrows, chan), 0), rows)
    lane_head = lax.broadcasted_iota(jnp.int32, (1, chan), 1) // hd

    def pair_bias(ready, get_row, put_row, wb, out):
        wide = wb[...].astype(F32)
        wide = jnp.concatenate([jnp.broadcast_to(wide[h:h + 1], (rows, chan)) for h in range(heads)], axis=0)
        bacc[...] = jnp.zeros_like(bacc)

        def step(i, carry):
            ready(i)
            rs = [LN_UNROLL * i + t for t in range(LN_UNROLL)]
            us = [norm(get_row(r)) for r in rs]
            total = sum(mm(jnp.where(row_of == r, wide, 0.0).astype(BF16), u, 1, 1) for r, u in zip(rs, us))
            if put_row is not None:
                for r, u in zip(rs, us):
                    put_row(r, u)
            bacc[...] += total
            return carry

        lax.fori_loop(0, rows // LN_UNROLL, step, 0)
        out[me] = bacc[...].astype(BF16)

    def bias_copy(buf, ss, rs, dev):
        return remote(buf.at[me], buf.at[me], ss, rs.at[me], dev)

    def by_distance(dist):
        return lax.rem(chip + ((dist + 1) // 2 if dist % 2 else chips - dist // 2), chips)

    def at(off):
        return lax.rem(chip + off + chips, chips)

    def bias_send(buf, ss, rs):
        bias_copy(buf, ss, rs, partner).start()
        for dist in range(1, chips):
            bias_copy(buf, ss, rs, by_distance(dist) * CORES + core).start()

    def bias_wait(buf, ss, rs, src):
        remote(buf.at[src], buf.at[src], ss, rs.at[src], partner).wait_recv()

    def forward(buf, ss, rs, c):
        src = c * CORES + core
        return remote(buf.at[src], buf.at[src], ss, rs.at[src], partner)

    def fetch(buf, ss, rs, c):
        bias_wait(buf, ss, rs, c * CORES + core)
        forward(buf, ss, rs, c).start()

    def sent(buf, ss, rs):
        remote(buf, buf, ss, rs, partner).wait_send()

    def put_u(r, u):
        u_s[r] = u

    w_loads[0].wait()
    with jax.named_scope("bias_rows"):
        pair_bias(lambda i: z_load(i).wait(), lambda r: z_ref[r], put_u, wb_s, brecv)
    with jax.named_scope("barrier"):
        pl.semaphore_wait(barrier, n - 1)
    bias_send(brecv, b_ss, b_rs)
    for cp in w_loads[1:]:
        cp.wait()


    def project(i, carry):
        for t in range(2):
            r = 2 * i + t
            u = u_s[r]
            pr = mm(u, wp_s[...])
            q_s[r] = pr[:, :chan].astype(BF16)
            kt_s[r] = pr[:, chan:2 * chan].T.astype(BF16)
            v_s[r] = pr[:, 2 * chan:3 * chan].astype(BF16)
            g_s[r] = sigmoid(pr[:, 3 * chan:])
        return carry

    with jax.named_scope("project"):
        lax.fori_loop(0, rows // 2, project, 0)

    def attention(qs, kts, vs, biases, gates, wo):
        nrow = qs[0].shape[0]
        qm = [jnp.concatenate([jnp.where(lane_head == h, q, jnp.zeros_like(q)) for h in range(heads)], axis=0) for q in qs]
        sc = [mm(a, kt) * scale + b[...] for a, kt, b in zip(qm, kts, biases)]
        pe = [jnp.exp(s - jnp.max(s, axis=-1, keepdims=True)) for s in sc]
        ls = [1.0 / jnp.sum(e, axis=-1, keepdims=True) for e in pe]
        os = [mm(e.astype(BF16), v) * l for e, v, l in zip(pe, vs, ls)]
        upds = []
        for o, gate in zip(os, gates):
            mix = sum(jnp.where(lane_head == h, o[h * nrow:(h + 1) * nrow], 0.0) for h in range(heads))
            upds.append(mm((mix * gate).astype(BF16), wo[...]))
        return upds

    def h_copy(dev, hf):
        return remote(hsend.at[pl.ds(dev * rows + hf * part, part)],
                      ht.at[pl.ds(hf * part, part), pl.ds(aligned(me * rows, rows), rows), :], h_ss, h_rs.at[hf], dev)

    wide = CORES * rows

    def start_block(cs, between):
        nc = len(cs)
        nq = nc * wide
        for h in range(heads):
            for k in range(nc * CORES):
                src = brecv[cs[k // CORES] * CORES + k % CORES, h * rows:(h + 1) * rows, :]
                bias_f[h * nq + k * rows:h * nq + (k + 1) * rows, :] = src.astype(F32)
        cols = [pl.ds(aligned(c * wide, wide), wide) for c in cs]
        bias = bias_f.at[pl.ds(0, heads * nq)]

        def attend(i, carry):
            rs = [ROW_UNROLL * i + t for t in range(ROW_UNROLL)]
            qs = [jnp.concatenate([q_s[r, sl, :] for sl in cols], axis=0) for r in rs]
            gates = [jnp.concatenate([g_s[r, sl, :] for sl in cols], axis=0) for r in rs]
            upds = attention(qs, [kt_s[r] for r in rs], [v_s[r] for r in rs], [bias] * len(rs), gates, wo_s)
            for r, upd in zip(rs, upds):
                z1 = jnp.concatenate([z_ref[r, sl, :] for sl in cols], axis=0) + upd
                for k, c in enumerate(cs):
                    z1_ref[pl.ds(aligned(r * seq + c * wide, wide), wide), :] = z1[k * wide:(k + 1) * wide]
                zb[pl.ds(aligned(r * (nq + PAD), PAD), nq), :] = z1
            return carry

        half = rows // ROW_UNROLL // 2
        with jax.named_scope("attend_a"):
            lax.fori_loop(0, half, attend, 0)
        with jax.named_scope("fetch_next"):
            between()
        with jax.named_scope("attend_b"):
            lax.fori_loop(half, 2 * half, attend, 0)
        for k, c in enumerate(cs):
            for j in range(wide):
                hsend[c * wide + j] = zb[pl.ds(k * wide + j, rows, stride=nq + PAD), :].astype(BF16)

    def wait_other(c):
        with jax.named_scope("wait_block"):
            bias_wait(brecv, b_ss, b_rs, c * CORES + other)

    def fetch_ring(dist):
        fetch(brecv, b_ss, b_rs, at(dist))
        if isinstance(dist, int):
            if 2 * dist % chips:
                fetch(brecv, b_ss, b_rs, at(-dist))
        else:
            @pl.when(2 * dist < chips)
            def _():
                fetch(brecv, b_ss, b_rs, at(-dist))

    def send_ring(cs, hf):
        for s in range(CORES):
            for c in cs:
                h_copy(c * CORES + s, hf).start()

    bias_wait(brecv, b_ss, b_rs, partner)
    start_block([chip], lambda: fetch_ring(1))
    for hf in range(HALVES):
        h_copy(partner, hf).start()

    def start_ring(dist, carry):
        cs = [at(dist), at(-dist)]
        for c in cs:
            wait_other(c)
        start_block(cs, lambda: fetch_ring(dist + 1))
        send_ring(cs, 0)
        for hf in range(1, HALVES):
            @pl.when(dist < HOLD_FROM)
            def _():
                send_ring(cs, hf)
        return carry

    far = chips // 2
    lax.fori_loop(1, far, start_ring, 0)
    wait_other(at(far))
    start_block([at(far)], lambda: None)
    send_ring([at(far)], 0)

    with jax.named_scope("bias_cols"):
        pair_bias(lambda i: None, lambda r: z1_ref[pl.ds(aligned(r * seq, seq), seq), :].astype(BF16).astype(F32), None, wb_e, erecv)
    bias_send(erecv, e_ss, e_rs)
    for hf in range(1, HALVES):
        for dist in range(HOLD_FROM, far):
            send_ring([at(dist), at(-dist)], hf)
        send_ring([at(far)], hf)
    ht[:, pl.ds(aligned(me * rows, rows), rows), :] = hsend[pl.ds(aligned(me * rows, rows), rows)]

    with jax.named_scope("wait_cols"):
        for dist in range(1, chips):
            fetch(erecv, e_ss, e_rs, by_distance(dist))
        for c in range(chips):
            bias_wait(erecv, e_ss, e_rs, c * CORES + other)

    def widen(h, carry):
        tall = jnp.concatenate([erecv[dev, pl.ds(aligned(h * rows, rows), rows), :] for dev in range(n)], axis=0)
        bias_e[pl.ds(aligned(h * seq, seq), seq), :] = tall.astype(F32).T
        return carry

    with jax.named_scope("widen"):
        lax.fori_loop(0, heads, widen, 0)

    def is_far(off):
        return int(min(off // CORES, chips - off // CORES) > 2)

    def d_copy(off, grp):
        dev = lax.rem(me // CORES * CORES + off // CORES * CORES, n) + (core if off % CORES == 0 else other)
        return remote(dsend.at[pl.ds(grp * COL_GROUP, COL_GROUP), pl.ds(aligned(dev * rows, rows), rows), :],
                      drecv.at[pl.ds(me * rows + grp * COL_GROUP, COL_GROUP)],
                      d_ss, d_rs.at[grp // (part // COL_GROUP), is_far(off)], dev)

    def end_cols(i, carry):
        js = [COL_UNROLL * i + t for t in range(COL_UNROLL)]
        hs = [ht[j] for j in js]
        us = [norm(h.astype(F32)) for h in hs]
        prs = [mm(u, wp_e[...]) for u in us]
        kts = [p[:, chan:2 * chan].T.astype(BF16) for p in prs]
        es = attention([p[:, :chan].astype(BF16) for p in prs], kts, [p[:, 2 * chan:3 * chan].astype(BF16) for p in prs],
                       [bias_e] * len(js), [sigmoid(p[:, 3 * chan:]) for p in prs], wo_e)
        z2 = [h.astype(F32) + e for h, e in zip(hs, es)]
        hid = [jnp.maximum(mm(norm(z), w1[...]), 0.0).astype(BF16) for z in z2]
        ts = [mm(x, w2[...]) for x in hid]
        for j, e, t in zip(js, es, ts):
            dsend[j] = (e + t).astype(BF16)
        return carry

    far_first = sorted(range(1, n), key=lambda off: -min(off // CORES, chips - off // CORES))
    per = COL_GROUP // COL_UNROLL

    def end_group(grp, carry):
        for hf in range(HALVES):
            @pl.when(grp == hf * (part // COL_GROUP))
            def _():
                with jax.named_scope("wait_h"):
                    whole = hsend.at[pl.ds(0, (n - 1) * part)]
                    remote(whole, whole, h_ss, h_rs.at[hf], partner).wait_recv()
        with jax.named_scope("end_cols"):
            lax.fori_loop(grp * per, (grp + 1) * per, end_cols, 0)
        for off in far_first:
            d_copy(off, grp).start()
        return carry

    lax.fori_loop(0, rows // COL_GROUP, end_group, 0)
    drecv[pl.ds(me * rows, rows)] = dsend[:, pl.ds(aligned(me * rows, rows), rows), :]

    pitch = rows + PAD
    with jax.named_scope("finish"):
        for hf in range(HALVES):
            def finish(first, k, carry):
                dev = at(first + k // CORES) * CORES + lax.rem(k, CORES)
                base = dev * (part * pitch)
                for t in range(part):
                    tmp[pl.ds(aligned(base + t * pitch, PAD), rows), :] = drecv[dev * rows + hf * part + t].astype(F32)
                for i in range(rows):
                    z1_ref[pl.ds(aligned(i * seq + dev * rows + hf * part, part), part), :] += tmp[pl.ds(base + i, part, stride=pitch), :]
                return carry

            for side, first, num in ((0, -2, 5), (1, 3, chips - 5)):
                arrived = drecv.at[pl.ds(0, (num * CORES - (1 - side)) * part)]
                remote(arrived, arrived, d_ss, d_rs.at[hf, side], partner).wait_recv()
                lax.fori_loop(0, num * CORES, functools.partial(finish, first), 0)

    with jax.named_scope("drain"):
        for buf, ss, rs in ((brecv, b_ss, b_rs), (erecv, e_ss, e_rs)):
            sent(buf.at[pl.ds(0, n - 1)], ss, rs.at[0])
        sent(hsend.at[pl.ds(0, (n - 1) * rows)], h_ss, h_rs.at[0])
        sent(dsend.at[pl.ds(0, n - 1)], d_ss, d_rs.at[0, 0])


def solution(mesh):
    row_spec = P(('dp', AXIS), None, None)
    n = mesh.shape[AXIS]

    def local_fn(z, *weights):
        rows, seq, chan = z.shape
        heads = weights[1].shape[0]
        hrows = heads * rows
        part = rows // HALVES
        nq = 2 * CORES * rows
        dma = pltpu.SemaphoreType.DMA
        vmem = pl.BlockSpec(memory_space=pltpu.VMEM)
        y = pl.pallas_call(
            functools.partial(kernel, n, rows, seq, heads),
            out_shape=jax.ShapeDtypeStruct((rows * seq, chan), F32),
            in_specs=[pl.BlockSpec(memory_space=pltpu.HBM)] * 9,
            out_specs=vmem,
            scratch_shapes=[pltpu.VMEM(z.shape, z.dtype)] + [pltpu.VMEM(w.shape, w.dtype) for w in weights] + [
                pltpu.VMEM((rows, seq, chan), BF16),
                pltpu.VMEM((rows, seq, chan), BF16),
                pltpu.VMEM((rows, chan, seq), BF16),
                pltpu.VMEM((rows, seq, chan), BF16),
                pltpu.VMEM((rows, seq, chan), F32),
                pltpu.VMEM((hrows, seq), F32),
                pltpu.VMEM((n, hrows, seq), BF16),
                pltpu.VMEM((heads * nq, seq), F32),
                pltpu.VMEM((rows * (nq + PAD), chan), F32),
                pltpu.VMEM((seq, rows, chan), BF16),
                pltpu.VMEM((rows, seq, chan), BF16),
                pltpu.VMEM((n, hrows, seq), BF16),
                pltpu.VMEM((heads * seq, seq), F32),
                pltpu.VMEM((rows, seq, chan), BF16),
                pltpu.VMEM((seq, rows, chan), BF16),
                pltpu.VMEM((n * part * (rows + PAD), chan), F32),
                dma((rows // LN_UNROLL,)), dma((len(weights),)),
                dma, dma((n,)), dma, dma((n,)), dma, dma((HALVES,)), dma, dma((HALVES, 2)),
            ],
            compiler_params=pltpu.CompilerParams(collective_id=0, has_side_effects=True, vmem_limit_bytes=40 * 2 ** 20),
        )(*[pltpu.with_memory_space_constraint(a, pltpu.HBM) for a in (z,) + weights])
        return y.reshape(rows, seq, chan)

    return jax.shard_map(local_fn, mesh=mesh, in_specs=(row_spec,) + (P(),) * 8, out_specs=row_spec, check_vma=False)
```

```python
import functools

import jax
import jax.numpy as jnp
from jax import lax
from jax.experimental import pallas as pl
from jax.experimental.pallas import tpu as pltpu
from jax.sharding import PartitionSpec as P

LN_EPS = 1e-5
F32, BF16 = jnp.float32, jnp.bfloat16
MESH = pl.DeviceIdType.MESH
AXIS = "sp"
CORES = 2
HALVES = 2
COL_GROUP = 2
HOLD_FROM = 2
ROW_UNROLL = 8
COL_UNROLL = 2
LN_UNROLL = 8
PROJ_UNROLL = 8
Z_ROWS = 4
PAD = 8


def norm(vals):
    mean_c = jnp.mean(vals, axis=-1, keepdims=True)
    centered = vals - mean_c
    variance = jnp.mean(centered * centered, axis=-1, keepdims=True)
    return (centered * lax.rsqrt(variance + LN_EPS)).astype(BF16)


def mm(a, b, ca=1, cb=0):
    return lax.dot_general(a, b, (((ca,), (cb,)), ((), ())), preferred_element_type=F32)


def sigmoid(x):
    return 1.0 / (1.0 + jnp.exp(-x))


def kernel(n, rows, seq, heads, z_hbm, wps_h, wbs_h, wos_h, wpe_h, wbe_h, woe_h, w1_h, w2_h,
           z1_ref,
           z_ref, wp_s, wb_s, wo_s, wp_e, wb_e, wo_e, w1, w2,
           u_s, q_s, kt_s, v_s, g_s, bacc, brecv, bias_f, zb, hsend, ht, erecv, bias_e, dsend, drecv, tmp,
           z_sem, w_sem, b_ss, b_rs, e_ss, e_rs, h_ss, h_rs, d_ss, d_rs):
    chan = wo_s.shape[0]
    hd = chan // heads
    scale = hd ** -0.5
    chips = n // CORES
    part = rows // HALVES
    me = lax.axis_index(AXIS)
    chip, core = me // CORES, lax.rem(me, CORES)
    other = CORES - 1 - core
    partner = chip * CORES + other
    hrows = heads * rows

    def remote(src, dst, ss, rs, dev):
        return pltpu.make_async_remote_copy(src_ref=src, dst_ref=dst, send_sem=ss, recv_sem=rs,
                                            device_id={AXIS: dev}, device_id_type=MESH)

    def aligned(i, k):
        return pl.multiple_of(i, k)

    barrier = pltpu.get_barrier_semaphore()
    for off in range(1, n):
        pl.semaphore_signal(barrier, 1, device_id={AXIS: lax.rem(me + off, n)}, device_id_type=MESH)

    def z_load(i):
        sl = pl.ds(i * Z_ROWS, Z_ROWS)
        return pltpu.make_async_copy(z_hbm.at[sl], z_ref.at[sl], z_sem.at[i])

    def z_row(r):
        return pltpu.make_async_copy(z_hbm.at[r], z_ref.at[r], z_sem.at[r // Z_ROWS])

    w_loads = [pltpu.make_async_copy(src, dst, w_sem.at[i]) for i, (src, dst) in enumerate(
        [(wbs_h, wb_s), (wps_h, wp_s), (wos_h, wo_s), (wbe_h, wb_e), (wpe_h, wp_e), (woe_h, wo_e), (w1_h, w1), (w2_h, w2)])]
    w_loads[0].start()
    for r in range(rows):
        z_row(r).start()
    for cp in w_loads[1:]:
        cp.start()

    row_of = lax.rem(lax.broadcasted_iota(jnp.int32, (hrows, chan), 0), rows)
    lane_head = lax.broadcasted_iota(jnp.int32, (1, chan), 1) // hd

    def pair_bias(ready, get_row, put_row, wb, out):
        wide = wb[...].astype(F32)
        wide = jnp.concatenate([jnp.broadcast_to(wide[h:h + 1], (rows, chan)) for h in range(heads)], axis=0)
        bacc[...] = jnp.zeros_like(bacc)

        def step(i, carry):
            ready(i)
            rs = [LN_UNROLL * i + t for t in range(LN_UNROLL)]
            us, total = [], 0.0
            for r in rs:
                us.append(norm(get_row(r)))
                total += mm(jnp.where(row_of == r, wide, 0.0).astype(BF16), us[-1], 1, 1)
            if put_row is not None:
                for r, u in zip(rs, us):
                    put_row(r, u)
            bacc[...] += total
            return carry

        lax.fori_loop(0, rows // LN_UNROLL, step, 0)
        out[me] = bacc[...].astype(BF16)

    def bias_copy(buf, ss, rs, dev):
        return remote(buf.at[me], buf.at[me], ss, rs.at[me], dev)

    def at(off):
        return lax.rem(chip + off + chips, chips)

    def bias_send(buf, ss, rs, both):
        bias_copy(buf, ss, rs, partner).start()
        for off in (1, -1):
            bias_copy(buf, ss, rs, at(off) * CORES + core).start()
        for off in (1, -1) if both else ():
            bias_copy(buf, ss, rs, at(off) * CORES + other).start()
        for off in (2, -2):
            bias_copy(buf, ss, rs, at(off) * CORES + core).start()

    def bias_wait(buf, ss, rs, src):
        remote(buf.at[src], buf.at[src], ss, rs.at[src], partner).wait_recv()

    def forward(buf, ss, rs, c):
        src = c * CORES + core
        return remote(buf.at[src], buf.at[src], ss, rs.at[src], partner)

    def fetch(buf, ss, rs, c):
        bias_wait(buf, ss, rs, c * CORES + core)
        forward(buf, ss, rs, c).start()

    def relay(buf, ss, rs):
        for sign in (1, -1):
            origin = at(-2 * sign) * CORES + core
            bias_wait(buf, ss, rs, origin)
            row = buf.at[origin]
            remote(row, row, ss, rs.at[origin], at(sign) * CORES + core).start()

            @pl.when(core == (1 - sign) // 2)
            def _():
                remote(row, row, ss, rs.at[origin], at(2 * sign) * CORES + core).start()
            forward(buf, ss, rs, at(-2 * sign)).start()

    def sent(buf, ss, rs):
        remote(buf, buf, ss, rs, partner).wait_send()

    def put_u(r, u):
        u_s[r] = u

    w_loads[0].wait()
    with jax.named_scope("bias_rows"):
        def ready(i):
            for t in range(LN_UNROLL // Z_ROWS):
                z_load(i * (LN_UNROLL // Z_ROWS) + t).wait()

        pair_bias(ready, lambda r: z_ref[r], put_u, wb_s, brecv)
    with jax.named_scope("barrier"):
        pl.semaphore_wait(barrier, n - 1)
    bias_send(brecv, b_ss, b_rs, True)
    for cp in w_loads[1:]:
        cp.wait()


    def project(i, carry):
        rs = [PROJ_UNROLL * i + t for t in range(PROJ_UNROLL)]
        prs = [mm(u_s[r], wp_s[...]) for r in rs]
        for r, pr in zip(rs, prs):
            q_s[r] = pr[:, :chan].astype(BF16)
            kt_s[r] = pr[:, chan:2 * chan].T.astype(BF16)
            v_s[r] = pr[:, 2 * chan:3 * chan].astype(BF16)
            g_s[r] = sigmoid(pr[:, 3 * chan:])
        return carry

    with jax.named_scope("project"):
        lax.fori_loop(0, rows // PROJ_UNROLL, project, 0)

    def attention(qs, kts, vs, biases, gates, wo):
        nrow = qs[0].shape[0]
        qm = [jnp.concatenate([jnp.where(lane_head == h, q, jnp.zeros_like(q)) for h in range(heads)], axis=0) for q in qs]
        sc = [mm(a, kt) * scale + b[...] for a, kt, b in zip(qm, kts, biases)]
        pe = [jnp.exp(s - jnp.max(s, axis=-1, keepdims=True)) for s in sc]
        ls = [1.0 / jnp.sum(e, axis=-1, keepdims=True) for e in pe]
        os = [mm(e.astype(BF16), v) * l for e, v, l in zip(pe, vs, ls)]
        upds = []
        for o, gate in zip(os, gates):
            mix = sum(jnp.where(lane_head == h, o[h * nrow:(h + 1) * nrow], 0.0) for h in range(heads))
            upds.append(mm((mix * gate).astype(BF16), wo[...]))
        return upds

    def h_copy(dev, hf):
        return remote(hsend.at[pl.ds(dev * rows + hf * part, part)],
                      ht.at[pl.ds(hf * part, part), pl.ds(aligned(me * rows, rows), rows), :], h_ss, h_rs.at[hf], dev)

    wide = CORES * rows

    def start_block(cs, between):
        nc = len(cs)
        nq = nc * wide
        for h in range(heads):
            for k in range(nc * CORES):
                src = brecv[cs[k // CORES] * CORES + k % CORES, h * rows:(h + 1) * rows, :]
                bias_f[h * nq + k * rows:h * nq + (k + 1) * rows, :] = src.astype(F32)
        cols = [pl.ds(aligned(c * wide, wide), wide) for c in cs]
        bias = bias_f.at[pl.ds(0, heads * nq)]

        def attend(i, carry):
            rs = [ROW_UNROLL * i + t for t in range(ROW_UNROLL)]
            qs = [jnp.concatenate([q_s[r, sl, :] for sl in cols], axis=0) for r in rs]
            gates = [jnp.concatenate([g_s[r, sl, :] for sl in cols], axis=0) for r in rs]
            upds = attention(qs, [kt_s[r] for r in rs], [v_s[r] for r in rs], [bias] * len(rs), gates, wo_s)
            for r, upd in zip(rs, upds):
                z1 = jnp.concatenate([z_ref[r, sl, :] for sl in cols], axis=0) + upd
                for k, c in enumerate(cs):
                    z1_ref[pl.ds(aligned(r * seq + c * wide, wide), wide), :] = z1[k * wide:(k + 1) * wide]
                zb[pl.ds(aligned(r * (nq + PAD), PAD), nq), :] = z1
            return carry

        half = rows // ROW_UNROLL // 2
        with jax.named_scope("attend_a"):
            lax.fori_loop(0, half, attend, 0)
        with jax.named_scope("fetch_next"):
            between()
        with jax.named_scope("attend_b"):
            lax.fori_loop(half, 2 * half, attend, 0)
        for k, c in enumerate(cs):
            for j in range(wide):
                hsend[c * wide + j] = zb[pl.ds(k * wide + j, rows, stride=nq + PAD), :].astype(BF16)

    def wait_other(c):
        with jax.named_scope("wait_block"):
            bias_wait(brecv, b_ss, b_rs, c * CORES + other)

    def fetch_ring(dist):
        fetch(brecv, b_ss, b_rs, at(dist))

        @pl.when(2 * dist < chips)
        def _():
            fetch(brecv, b_ss, b_rs, at(-dist))

    def send_ring(cs, hf):
        for s in range(CORES):
            for c in cs:
                h_copy(c * CORES + s, hf).start()

    bias_wait(brecv, b_ss, b_rs, partner)
    start_block([chip], lambda: None)
    for off in (1, -1):
        bias_wait(brecv, b_ss, b_rs, at(off) * CORES + core)
    for hf in range(HALVES):
        h_copy(partner, hf).start()

    def start_ring(dist, carry):
        cs = [at(dist), at(-dist)]
        for c in cs:
            wait_other(c)
        def between():
            @pl.when(dist == 1)
            def _():
                relay(brecv, b_ss, b_rs)

            @pl.when(dist > 1)
            def _():
                fetch_ring(dist + 1)

        start_block(cs, between)
        send_ring(cs, 0)
        for hf in range(1, HALVES):
            @pl.when(dist < HOLD_FROM)
            def _():
                send_ring(cs, hf)
        return carry

    far = chips // 2
    lax.fori_loop(1, far, start_ring, 0)
    wait_other(at(far))
    start_block([at(far)], lambda: None)

    with jax.named_scope("bias_cols"):
        pair_bias(lambda i: None, lambda r: z1_ref[pl.ds(aligned(r * seq, seq), seq), :].astype(BF16).astype(F32), None, wb_e, erecv)
    bias_send(erecv, e_ss, e_rs, False)
    send_ring([at(far)], 0)
    ht[:, pl.ds(aligned(me * rows, rows), rows), :] = hsend[pl.ds(aligned(me * rows, rows), rows)]

    with jax.named_scope("wait_cols"):
        relay(erecv, e_ss, e_rs)
        for hf in range(1, HALVES):
            for dist in range(HOLD_FROM, far):
                send_ring([at(dist), at(-dist)], hf)
            send_ring([at(far)], hf)
        for off in (1, -1, 3, -3, 4):
            fetch(erecv, e_ss, e_rs, at(off))
        for c in range(chips):
            bias_wait(erecv, e_ss, e_rs, c * CORES + other)

    def widen(h, carry):
        tall = jnp.concatenate([erecv[dev, pl.ds(aligned(h * rows, rows), rows), :] for dev in range(n)], axis=0)
        bias_e[pl.ds(aligned(h * seq, seq), seq), :] = tall.astype(F32).T
        return carry

    with jax.named_scope("widen"):
        lax.fori_loop(0, heads, widen, 0)

    def is_far(off):
        return int(min(off // CORES, chips - off // CORES) > 2)

    def d_copy(off, grp):
        dev = lax.rem(me // CORES * CORES + off // CORES * CORES, n) + (core if off % CORES == 0 else other)
        return remote(dsend.at[pl.ds(grp * COL_GROUP, COL_GROUP), pl.ds(aligned(dev * rows, rows), rows), :],
                      drecv.at[pl.ds(me * rows + grp * COL_GROUP, COL_GROUP)],
                      d_ss, d_rs.at[grp // (part // COL_GROUP), is_far(off)], dev)

    def end_cols(i, carry):
        js = [COL_UNROLL * i + t for t in range(COL_UNROLL)]
        hs = [ht[j] for j in js]
        us = [norm(h.astype(F32)) for h in hs]
        prs = [mm(u, wp_e[...]) for u in us]
        kts = [p[:, chan:2 * chan].T.astype(BF16) for p in prs]
        es = attention([p[:, :chan].astype(BF16) for p in prs], kts, [p[:, 2 * chan:3 * chan].astype(BF16) for p in prs],
                       [bias_e] * len(js), [sigmoid(p[:, 3 * chan:]) for p in prs], wo_e)
        z2 = [h.astype(F32) + e for h, e in zip(hs, es)]
        hid = [jnp.maximum(mm(norm(z), w1[...]), 0.0).astype(BF16) for z in z2]
        ts = [mm(x, w2[...]) for x in hid]
        for j, e, t in zip(js, es, ts):
            dsend[j] = (e + t).astype(BF16)
        return carry

    far_first = sorted(range(1, n), key=lambda off: -min(off // CORES, chips - off // CORES))
    per = COL_GROUP // COL_UNROLL

    def end_group(grp, carry):
        for hf in range(HALVES):
            @pl.when(grp == hf * (part // COL_GROUP))
            def _():
                with jax.named_scope("wait_h"):
                    whole = hsend.at[pl.ds(0, (n - 1) * part)]
                    remote(whole, whole, h_ss, h_rs.at[hf], partner).wait_recv()
        with jax.named_scope("end_cols"):
            lax.fori_loop(grp * per, (grp + 1) * per, end_cols, 0)
        for off in far_first:
            d_copy(off, grp).start()
        return carry

    lax.fori_loop(0, rows // COL_GROUP, end_group, 0)
    drecv[pl.ds(me * rows, rows)] = dsend[:, pl.ds(aligned(me * rows, rows), rows), :]

    pitch = rows + PAD
    with jax.named_scope("finish"):
        for hf in range(HALVES):
            def finish(first, k, carry):
                dev = at(first + k // CORES) * CORES + lax.rem(k, CORES)
                base = dev * (part * pitch)
                for t in range(part):
                    tmp[pl.ds(aligned(base + t * pitch, PAD), rows), :] = drecv[dev * rows + hf * part + t].astype(F32)
                for i in range(rows):
                    z1_ref[pl.ds(aligned(i * seq + dev * rows + hf * part, part), part), :] += tmp[pl.ds(base + i, part, stride=pitch), :]
                return carry

            for side, first, num in ((0, -2, 5), (1, 3, chips - 5)):
                arrived = drecv.at[pl.ds(0, (num * CORES - (1 - side)) * part)]
                remote(arrived, arrived, d_ss, d_rs.at[hf, side], partner).wait_recv()
                lax.fori_loop(0, num * CORES, functools.partial(finish, first), 0)

    with jax.named_scope("drain"):
        for buf, ss, rs in ((brecv, b_ss, b_rs), (erecv, e_ss, e_rs)):
            sent(buf.at[pl.ds(0, n - 1)], ss, rs.at[0])
        sent(hsend.at[pl.ds(0, (n - 1) * rows)], h_ss, h_rs.at[0])
        sent(dsend.at[pl.ds(0, n - 1)], d_ss, d_rs.at[0, 0])


def solution(mesh):
    row_spec = P(('dp', AXIS), None, None)
    n = mesh.shape[AXIS]

    def local_fn(z, *weights):
        rows, seq, chan = z.shape
        heads = weights[1].shape[0]
        hrows = heads * rows
        part = rows // HALVES
        nq = 2 * CORES * rows
        dma = pltpu.SemaphoreType.DMA
        vmem = pl.BlockSpec(memory_space=pltpu.VMEM)
        y = pl.pallas_call(
            functools.partial(kernel, n, rows, seq, heads),
            out_shape=jax.ShapeDtypeStruct((rows * seq, chan), F32),
            in_specs=[pl.BlockSpec(memory_space=pltpu.HBM)] * 9,
            out_specs=vmem,
            scratch_shapes=[pltpu.VMEM(z.shape, z.dtype)] + [pltpu.VMEM(w.shape, w.dtype) for w in weights] + [
                pltpu.VMEM((rows, seq, chan), BF16),
                pltpu.VMEM((rows, seq, chan), BF16),
                pltpu.VMEM((rows, chan, seq), BF16),
                pltpu.VMEM((rows, seq, chan), BF16),
                pltpu.VMEM((rows, seq, chan), F32),
                pltpu.VMEM((hrows, seq), F32),
                pltpu.VMEM((n, hrows, seq), BF16),
                pltpu.VMEM((heads * nq, seq), F32),
                pltpu.VMEM((rows * (nq + PAD), chan), F32),
                pltpu.VMEM((seq, rows, chan), BF16),
                pltpu.VMEM((rows, seq, chan), BF16),
                pltpu.VMEM((n, hrows, seq), BF16),
                pltpu.VMEM((heads * seq, seq), F32),
                pltpu.VMEM((rows, seq, chan), BF16),
                pltpu.VMEM((seq, rows, chan), BF16),
                pltpu.VMEM((n * part * (rows + PAD), chan), F32),
                dma((rows // Z_ROWS,)), dma((len(weights),)),
                dma, dma((n,)), dma, dma((n,)), dma, dma((HALVES,)), dma, dma((HALVES, 2)),
            ],
            compiler_params=pltpu.CompilerParams(collective_id=0, has_side_effects=True, vmem_limit_bytes=40 * 2 ** 20),
        )(*[pltpu.with_memory_space_constraint(a, pltpu.HBM) for a in (z,) + weights])
        return y.reshape(rows, seq, chan)

    return jax.shard_map(local_fn, mesh=mesh, in_specs=(row_spec,) + (P(),) * 8, out_specs=row_spec, check_vma=False)
```

```python
import functools

import jax
import jax.numpy as jnp
from jax import lax
from jax.experimental import pallas as pl
from jax.experimental.pallas import tpu as pltpu
from jax.sharding import PartitionSpec as P

LN_EPS = 1e-5
F32, BF16 = jnp.float32, jnp.bfloat16
MESH = pl.DeviceIdType.MESH
AXIS = "sp"
CORES = 2
HALVES = 2
COL_GROUP = 2
HOLD_FROM = 2
ROW_UNROLL = 8
COL_UNROLL = 2
LN_UNROLL = 8
PROJ_UNROLL = 8
Z_ROWS = 4
PAD = 8


def norm(vals):
    mean_c = jnp.mean(vals, axis=-1, keepdims=True)
    centered = vals - mean_c
    variance = jnp.mean(centered * centered, axis=-1, keepdims=True)
    return (centered * lax.rsqrt(variance + LN_EPS)).astype(BF16)


def mm(a, b, ca=1, cb=0):
    return lax.dot_general(a, b, (((ca,), (cb,)), ((), ())), preferred_element_type=F32)


def sigmoid(x):
    return 1.0 / (1.0 + jnp.exp(-x))


def kernel(n, rows, seq, heads, z_hbm, wps_h, wbs_h, wos_h, wpe_h, wbe_h, woe_h, w1_h, w2_h,
           z1_ref,
           z_ref, wp_s, wb_s, wo_s, wp_e, wb_e, wo_e, w1, w2,
           u_s, q_s, kt_s, v_s, g_s, bacc, brecv, bias_f, zb, hsend, ht, erecv, bias_e, dsend, drecv, tmp,
           z_sem, w_sem, b_ss, b_rs, e_ss, e_rs, h_ss, h_rs, d_ss, d_rs):
    chan = wo_s.shape[0]
    hd = chan // heads
    scale = hd ** -0.5
    chips = n // CORES
    part = rows // HALVES
    me = lax.axis_index(AXIS)
    chip, core = me // CORES, lax.rem(me, CORES)
    other = CORES - 1 - core
    partner = chip * CORES + other
    hrows = heads * rows

    def remote(src, dst, ss, rs, dev):
        return pltpu.make_async_remote_copy(src_ref=src, dst_ref=dst, send_sem=ss, recv_sem=rs,
                                            device_id={AXIS: dev}, device_id_type=MESH)

    def aligned(i, k):
        return pl.multiple_of(i, k)

    barrier = pltpu.get_barrier_semaphore()
    greeted = [partner] + [lax.rem(chip + off + chips, chips) * CORES + s for off in (1, -1, 2, -2) for s in range(CORES)]
    for dev in greeted:
        pl.semaphore_signal(barrier, 1, device_id={AXIS: dev}, device_id_type=MESH)

    def z_load(i):
        sl = pl.ds(i * Z_ROWS, Z_ROWS)
        return pltpu.make_async_copy(z_hbm.at[sl], z_ref.at[sl], z_sem.at[i])

    def z_row(r):
        return pltpu.make_async_copy(z_hbm.at[r], z_ref.at[r], z_sem.at[r // Z_ROWS])

    w_loads = [pltpu.make_async_copy(src, dst, w_sem.at[i]) for i, (src, dst) in enumerate(
        [(wbs_h, wb_s), (wps_h, wp_s), (wos_h, wo_s), (wbe_h, wb_e), (wpe_h, wp_e), (woe_h, wo_e), (w1_h, w1), (w2_h, w2)])]
    w_loads[0].start()
    for r in range(rows):
        z_row(r).start()
    for cp in w_loads[1:]:
        cp.start()

    row_of = lax.rem(lax.broadcasted_iota(jnp.int32, (hrows, chan), 0), rows)
    lane_head = lax.broadcasted_iota(jnp.int32, (1, chan), 1) // hd

    def pair_bias(ready, get_row, put_row, wb, out):
        wide = wb[...].astype(F32)
        wide = jnp.concatenate([jnp.broadcast_to(wide[h:h + 1], (rows, chan)) for h in range(heads)], axis=0)
        bacc[...] = jnp.zeros_like(bacc)

        def step(i, carry):
            ready(i)
            rs = [LN_UNROLL * i + t for t in range(LN_UNROLL)]
            us, total = [], 0.0
            for r in rs:
                us.append(norm(get_row(r)))
                total += mm(jnp.where(row_of == r, wide, 0.0).astype(BF16), us[-1], 1, 1)
            if put_row is not None:
                for r, u in zip(rs, us):
                    put_row(r, u)
            bacc[...] += total
            return carry

        lax.fori_loop(0, rows // LN_UNROLL, step, 0)
        out[me] = bacc[...].astype(BF16)

    def bias_copy(buf, ss, rs, dev):
        return remote(buf.at[me], buf.at[me], ss, rs.at[me], dev)

    def at(off):
        return lax.rem(chip + off + chips, chips)

    def bias_send(buf, ss, rs, both):
        bias_copy(buf, ss, rs, partner).start()
        for off in (1, -1):
            bias_copy(buf, ss, rs, at(off) * CORES + core).start()
        for off in (1, -1) if both else ():
            bias_copy(buf, ss, rs, at(off) * CORES + other).start()
        for off in (2, -2):
            bias_copy(buf, ss, rs, at(off) * CORES + core).start()

    def bias_wait(buf, ss, rs, src):
        remote(buf.at[src], buf.at[src], ss, rs.at[src], partner).wait_recv()

    def forward(buf, ss, rs, c):
        src = c * CORES + core
        return remote(buf.at[src], buf.at[src], ss, rs.at[src], partner)

    def fetch(buf, ss, rs, c):
        bias_wait(buf, ss, rs, c * CORES + core)
        forward(buf, ss, rs, c).start()

    def relay(buf, ss, rs):
        for sign in (1, -1):
            origin = at(-2 * sign) * CORES + core
            bias_wait(buf, ss, rs, origin)
            row = buf.at[origin]
            remote(row, row, ss, rs.at[origin], at(sign) * CORES + core).start()

            @pl.when(core == (1 - sign) // 2)
            def _():
                remote(row, row, ss, rs.at[origin], at(2 * sign) * CORES + core).start()
            forward(buf, ss, rs, at(-2 * sign)).start()

    def sent(buf, ss, rs):
        remote(buf, buf, ss, rs, partner).wait_send()

    def put_u(r, u):
        u_s[r] = u

    w_loads[0].wait()
    with jax.named_scope("bias_rows"):
        def ready(i):
            for t in range(LN_UNROLL // Z_ROWS):
                z_load(i * (LN_UNROLL // Z_ROWS) + t).wait()

        pair_bias(ready, lambda r: z_ref[r], put_u, wb_s, brecv)
    with jax.named_scope("barrier"):
        pl.semaphore_wait(barrier, len(greeted))
    bias_send(brecv, b_ss, b_rs, True)
    for cp in w_loads[1:]:
        cp.wait()


    def project(i, carry):
        rs = [PROJ_UNROLL * i + t for t in range(PROJ_UNROLL)]
        prs = [mm(u_s[r], wp_s[...]) for r in rs]
        for r, pr in zip(rs, prs):
            q_s[r] = pr[:, :chan].astype(BF16)
            kt_s[r] = pr[:, chan:2 * chan].T.astype(BF16)
            v_s[r] = pr[:, 2 * chan:3 * chan].astype(BF16)
            g_s[r] = sigmoid(pr[:, 3 * chan:])
        return carry

    with jax.named_scope("project"):
        lax.fori_loop(0, rows // PROJ_UNROLL, project, 0)

    def attention(qs, kts, vs, biases, gates, wo):
        nrow = qs[0].shape[0]
        qm = [jnp.concatenate([jnp.where(lane_head == h, q, jnp.zeros_like(q)) for h in range(heads)], axis=0) for q in qs]
        sc = [mm(a, kt) * scale + b[...] for a, kt, b in zip(qm, kts, biases)]
        pe = [jnp.exp(s - jnp.max(s, axis=-1, keepdims=True)) for s in sc]
        ls = [1.0 / jnp.sum(e, axis=-1, keepdims=True) for e in pe]
        os = [mm(e.astype(BF16), v) * l for e, v, l in zip(pe, vs, ls)]
        upds = []
        for o, gate in zip(os, gates):
            mix = sum(jnp.where(lane_head == h, o[h * nrow:(h + 1) * nrow], 0.0) for h in range(heads))
            upds.append(mm((mix * gate).astype(BF16), wo[...]))
        return upds

    def h_copy(dev, hf):
        return remote(hsend.at[pl.ds(dev * rows + hf * part, part)],
                      ht.at[pl.ds(hf * part, part), pl.ds(aligned(me * rows, rows), rows), :], h_ss, h_rs.at[hf], dev)

    wide = CORES * rows

    def start_block(cs, between):
        nc = len(cs)
        nq = nc * wide
        for h in range(heads):
            for k in range(nc * CORES):
                src = brecv[cs[k // CORES] * CORES + k % CORES, h * rows:(h + 1) * rows, :]
                bias_f[h * nq + k * rows:h * nq + (k + 1) * rows, :] = src.astype(F32)
        cols = [pl.ds(aligned(c * wide, wide), wide) for c in cs]
        bias = bias_f.at[pl.ds(0, heads * nq)]

        def attend(i, carry):
            rs = [ROW_UNROLL * i + t for t in range(ROW_UNROLL)]
            qs = [jnp.concatenate([q_s[r, sl, :] for sl in cols], axis=0) for r in rs]
            gates = [jnp.concatenate([g_s[r, sl, :] for sl in cols], axis=0) for r in rs]
            upds = attention(qs, [kt_s[r] for r in rs], [v_s[r] for r in rs], [bias] * len(rs), gates, wo_s)
            for r, upd in zip(rs, upds):
                z1 = jnp.concatenate([z_ref[r, sl, :] for sl in cols], axis=0) + upd
                for k, c in enumerate(cs):
                    z1_ref[pl.ds(aligned(r * seq + c * wide, wide), wide), :] = z1[k * wide:(k + 1) * wide]
                zb[pl.ds(aligned(r * (nq + PAD), PAD), nq), :] = z1
            return carry

        half = rows // ROW_UNROLL // 2
        with jax.named_scope("attend_a"):
            lax.fori_loop(0, half, attend, 0)
        with jax.named_scope("fetch_next"):
            between()
        with jax.named_scope("attend_b"):
            lax.fori_loop(half, 2 * half, attend, 0)
        for k, c in enumerate(cs):
            for j in range(wide):
                hsend[c * wide + j] = zb[pl.ds(k * wide + j, rows, stride=nq + PAD), :].astype(BF16)

    def wait_other(c):
        with jax.named_scope("wait_block"):
            bias_wait(brecv, b_ss, b_rs, c * CORES + other)

    def fetch_ring(dist):
        fetch(brecv, b_ss, b_rs, at(dist))

        @pl.when(2 * dist < chips)
        def _():
            fetch(brecv, b_ss, b_rs, at(-dist))

    def send_ring(cs, hf):
        for s in range(CORES):
            for c in cs:
                h_copy(c * CORES + s, hf).start()

    bias_wait(brecv, b_ss, b_rs, partner)
    start_block([chip], lambda: None)
    for off in (1, -1):
        bias_wait(brecv, b_ss, b_rs, at(off) * CORES + core)
    for hf in range(HALVES):
        h_copy(partner, hf).start()

    def start_ring(dist, carry):
        cs = [at(dist), at(-dist)]
        for c in cs:
            wait_other(c)
        def between():
            @pl.when(dist == 1)
            def _():
                relay(brecv, b_ss, b_rs)

            @pl.when(dist > 1)
            def _():
                fetch_ring(dist + 1)

        start_block(cs, between)
        send_ring(cs, 0)
        for hf in range(1, HALVES):
            @pl.when(dist < HOLD_FROM)
            def _():
                send_ring(cs, hf)
        return carry

    far = chips // 2
    lax.fori_loop(1, far, start_ring, 0)
    wait_other(at(far))
    start_block([at(far)], lambda: None)

    with jax.named_scope("bias_cols"):
        pair_bias(lambda i: None, lambda r: z1_ref[pl.ds(aligned(r * seq, seq), seq), :].astype(BF16).astype(F32), None, wb_e, erecv)
    bias_send(erecv, e_ss, e_rs, False)
    send_ring([at(far)], 0)
    ht[:, pl.ds(aligned(me * rows, rows), rows), :] = hsend[pl.ds(aligned(me * rows, rows), rows)]

    with jax.named_scope("wait_cols"):
        relay(erecv, e_ss, e_rs)
        for hf in range(1, HALVES):
            for dist in range(HOLD_FROM, far):
                send_ring([at(dist), at(-dist)], hf)
            send_ring([at(far)], hf)
        for off in (1, -1, 3, -3, 4):
            fetch(erecv, e_ss, e_rs, at(off))
        for c in range(chips):
            bias_wait(erecv, e_ss, e_rs, c * CORES + other)

    def widen(h, carry):
        tall = jnp.concatenate([erecv[dev, pl.ds(aligned(h * rows, rows), rows), :] for dev in range(n)], axis=0)
        bias_e[pl.ds(aligned(h * seq, seq), seq), :] = tall.astype(F32).T
        return carry

    with jax.named_scope("widen"):
        lax.fori_loop(0, heads, widen, 0)

    def is_far(off):
        return int(min(off // CORES, chips - off // CORES) > 2)

    def d_copy(off, grp):
        dev = lax.rem(me // CORES * CORES + off // CORES * CORES, n) + (core if off % CORES == 0 else other)
        return remote(dsend.at[pl.ds(grp * COL_GROUP, COL_GROUP), pl.ds(aligned(dev * rows, rows), rows), :],
                      drecv.at[pl.ds(me * rows + grp * COL_GROUP, COL_GROUP)],
                      d_ss, d_rs.at[grp // (part // COL_GROUP), is_far(off)], dev)

    def end_cols(i, carry):
        js = [COL_UNROLL * i + t for t in range(COL_UNROLL)]
        hs = [ht[j] for j in js]
        us = [norm(h.astype(F32)) for h in hs]
        prs = [mm(u, wp_e[...]) for u in us]
        kts = [p[:, chan:2 * chan].T.astype(BF16) for p in prs]
        es = attention([p[:, :chan].astype(BF16) for p in prs], kts, [p[:, 2 * chan:3 * chan].astype(BF16) for p in prs],
                       [bias_e] * len(js), [sigmoid(p[:, 3 * chan:]) for p in prs], wo_e)
        z2 = [h.astype(F32) + e for h, e in zip(hs, es)]
        hid = [jnp.maximum(mm(norm(z), w1[...]), 0.0).astype(BF16) for z in z2]
        ts = [mm(x, w2[...]) for x in hid]
        for j, e, t in zip(js, es, ts):
            dsend[j] = (e + t).astype(BF16)
        return carry

    far_first = sorted(range(1, n), key=lambda off: -min(off // CORES, chips - off // CORES))
    per = COL_GROUP // COL_UNROLL

    def end_group(grp, carry):
        for hf in range(HALVES):
            @pl.when(grp == hf * (part // COL_GROUP))
            def _():
                with jax.named_scope("wait_h"):
                    whole = hsend.at[pl.ds(0, (n - 1) * part)]
                    remote(whole, whole, h_ss, h_rs.at[hf], partner).wait_recv()
        with jax.named_scope("end_cols"):
            lax.fori_loop(grp * per, (grp + 1) * per, end_cols, 0)
        for off in far_first:
            d_copy(off, grp).start()
        return carry

    lax.fori_loop(0, rows // COL_GROUP, end_group, 0)
    drecv[pl.ds(me * rows, rows)] = dsend[:, pl.ds(aligned(me * rows, rows), rows), :]

    pitch = rows + PAD
    with jax.named_scope("finish"):
        for hf in range(HALVES):
            def finish(first, k, carry):
                dev = at(first + k // CORES) * CORES + lax.rem(k, CORES)
                base = dev * (part * pitch)
                for t in range(part):
                    tmp[pl.ds(aligned(base + t * pitch, PAD), rows), :] = drecv[dev * rows + hf * part + t].astype(F32)
                for i in range(rows):
                    z1_ref[pl.ds(aligned(i * seq + dev * rows + hf * part, part), part), :] += tmp[pl.ds(base + i, part, stride=pitch), :]
                return carry

            for side, first, num in ((0, -2, 5), (1, 3, chips - 5)):
                arrived = drecv.at[pl.ds(0, (num * CORES - (1 - side)) * part)]
                remote(arrived, arrived, d_ss, d_rs.at[hf, side], partner).wait_recv()
                lax.fori_loop(0, num * CORES, functools.partial(finish, first), 0)

    with jax.named_scope("drain"):
        for buf, ss, rs in ((brecv, b_ss, b_rs), (erecv, e_ss, e_rs)):
            sent(buf.at[pl.ds(0, n - 1)], ss, rs.at[0])
        sent(hsend.at[pl.ds(0, (n - 1) * rows)], h_ss, h_rs.at[0])
        sent(dsend.at[pl.ds(0, n - 1)], d_ss, d_rs.at[0, 0])


def solution(mesh):
    row_spec = P(('dp', AXIS), None, None)
    n = mesh.shape[AXIS]

    def local_fn(z, *weights):
        rows, seq, chan = z.shape
        heads = weights[1].shape[0]
        hrows = heads * rows
        part = rows // HALVES
        nq = 2 * CORES * rows
        dma = pltpu.SemaphoreType.DMA
        vmem = pl.BlockSpec(memory_space=pltpu.VMEM)
        y = pl.pallas_call(
            functools.partial(kernel, n, rows, seq, heads),
            out_shape=jax.ShapeDtypeStruct((rows * seq, chan), F32),
            in_specs=[pl.BlockSpec(memory_space=pltpu.HBM)] * 9,
            out_specs=vmem,
            scratch_shapes=[pltpu.VMEM(z.shape, z.dtype)] + [pltpu.VMEM(w.shape, w.dtype) for w in weights] + [
                pltpu.VMEM((rows, seq, chan), BF16),
                pltpu.VMEM((rows, seq, chan), BF16),
                pltpu.VMEM((rows, chan, seq), BF16),
                pltpu.VMEM((rows, seq, chan), BF16),
                pltpu.VMEM((rows, seq, chan), F32),
                pltpu.VMEM((hrows, seq), F32),
                pltpu.VMEM((n, hrows, seq), BF16),
                pltpu.VMEM((heads * nq, seq), F32),
                pltpu.VMEM((rows * (nq + PAD), chan), F32),
                pltpu.VMEM((seq, rows, chan), BF16),
                pltpu.VMEM((rows, seq, chan), BF16),
                pltpu.VMEM((n, hrows, seq), BF16),
                pltpu.VMEM((heads * seq, seq), F32),
                pltpu.VMEM((rows, seq, chan), BF16),
                pltpu.VMEM((seq, rows, chan), BF16),
                pltpu.VMEM((n * part * (rows + PAD), chan), F32),
                dma((rows // Z_ROWS,)), dma((len(weights),)),
                dma, dma((n,)), dma, dma((n,)), dma, dma((HALVES,)), dma, dma((HALVES, 2)),
            ],
            compiler_params=pltpu.CompilerParams(collective_id=0, has_side_effects=True, vmem_limit_bytes=40 * 2 ** 20),
        )(*[pltpu.with_memory_space_constraint(a, pltpu.HBM) for a in (z,) + weights])
        return y.reshape(rows, seq, chan)

    return jax.shard_map(local_fn, mesh=mesh, in_specs=(row_spec,) + (P(),) * 8, out_specs=row_spec, check_vma=False)
```

```python
import functools

import jax
import jax.numpy as jnp
from jax import lax
from jax.experimental import pallas as pl
from jax.experimental.pallas import tpu as pltpu
from jax.sharding import PartitionSpec as P

LN_EPS = 1e-5
F32, BF16 = jnp.float32, jnp.bfloat16
MESH = pl.DeviceIdType.MESH
AXIS = "sp"
CORES = 2
HALVES = 2
COL_GROUP = 2
HOLD_FROM = 2
ROW_UNROLL = 8
COL_UNROLL = 2
LN_ROWS = 4
PROJ_UNROLL = 8
PAD = 8


def norm(vals):
    mean_c = jnp.mean(vals, axis=-1, keepdims=True)
    centered = vals - mean_c
    variance = jnp.mean(centered * centered, axis=-1, keepdims=True)
    return (centered * lax.rsqrt(variance + LN_EPS)).astype(BF16)


def mm(a, b, ca=1, cb=0):
    return lax.dot_general(a, b, (((ca,), (cb,)), ((), ())), preferred_element_type=F32)


def sigmoid(x):
    return 1.0 / (1.0 + jnp.exp(-x))


def kernel(n, rows, seq, heads, z_hbm, wps_h, wbs_h, wos_h, wpe_h, wbe_h, woe_h, w1_h, w2_h,
           z1_ref,
           z_ref, wp_s, wb_s, wo_s, wp_e, wb_e, wo_e, w1, w2,
           u_s, q_s, kt_s, v_s, g_s, cen_a, cen_b, brecv, bias_f, zb, hsend, ht, erecv, bias_e, dsend, drecv, tmp,
           z_sem, w_sem, b_ss, b_rs, e_ss, e_rs, h_ss, h_rs, d_ss, d_rs):
    cen = (cen_a, cen_b)
    chan = wo_s.shape[0]
    hd = chan // heads
    scale = hd ** -0.5
    chips = n // CORES
    part = rows // HALVES
    me = lax.axis_index(AXIS)
    chip, core = me // CORES, lax.rem(me, CORES)
    other = CORES - 1 - core
    partner = chip * CORES + other
    hrows = heads * rows

    def remote(src, dst, ss, rs, dev):
        return pltpu.make_async_remote_copy(src_ref=src, dst_ref=dst, send_sem=ss, recv_sem=rs,
                                            device_id={AXIS: dev}, device_id_type=MESH)

    def aligned(i, k):
        return pl.multiple_of(i, k)

    def z_load(i):
        sl = pl.ds(i * LN_ROWS, LN_ROWS)
        return pltpu.make_async_copy(z_hbm.at[sl], z_ref.at[sl], z_sem.at[i])

    def z_row(r):
        return pltpu.make_async_copy(z_hbm.at[r], z_ref.at[r], z_sem.at[r // LN_ROWS])

    w_loads = [pltpu.make_async_copy(src, dst, w_sem.at[i]) for i, (src, dst) in enumerate(
        [(wbs_h, wb_s), (wps_h, wp_s), (wos_h, wo_s), (wbe_h, wb_e), (wpe_h, wp_e), (woe_h, wo_e), (w1_h, w1), (w2_h, w2)])]
    w_loads[0].start()
    for r in range(rows):
        z_row(r).start()
    for cp in w_loads[1:]:
        cp.start()

    barrier = pltpu.get_barrier_semaphore()
    greeted = [partner] + [lax.rem(chip + off + chips, chips) * CORES + s for off in (1, -1, 2, -2) for s in range(CORES)]
    for dev in greeted:
        pl.semaphore_signal(barrier, 1, device_id={AXIS: dev}, device_id_type=MESH)

    row_of = lax.rem(lax.broadcasted_iota(jnp.int32, (hrows, chan), 0), rows)
    lane_head = lax.broadcasted_iota(jnp.int32, (1, chan), 1) // hd

    def pair_bias(ready, get_row, put_row, wb, out):
        wide = wb[...].astype(F32)
        wide = jnp.concatenate([jnp.broadcast_to(wide[h:h + 1], (rows, chan)) for h in range(heads)], axis=0)
        total = jnp.zeros((hrows, seq), F32)
        steps = rows // LN_ROWS
        for i in range(steps + 1):
            if i < steps:
                ready(i)
                for t in range(LN_ROWS):
                    vals = get_row(i * LN_ROWS + t)
                    cen[i % 2][t] = vals - jnp.mean(vals, axis=-1, keepdims=True)
            if i:
                for t in range(LN_ROWS):
                    r = (i - 1) * LN_ROWS + t
                    centered = cen[(i - 1) % 2][t]
                    variance = jnp.mean(centered * centered, axis=-1, keepdims=True)
                    u = (centered * lax.rsqrt(variance + LN_EPS)).astype(BF16)
                    if put_row is not None:
                        put_row(r, u)
                    total += mm(jnp.where(row_of == r, wide, 0.0).astype(BF16), u, 1, 1)
        out[me] = total.astype(BF16)

    def bias_copy(buf, ss, rs, dev):
        return remote(buf.at[me], buf.at[me], ss, rs.at[me], dev)

    def at(off):
        return lax.rem(chip + off + chips, chips)

    def bias_send(buf, ss, rs, both):
        bias_copy(buf, ss, rs, partner).start()
        for off in (1, -1):
            bias_copy(buf, ss, rs, at(off) * CORES + core).start()
        for off in (1, -1) if both else ():
            bias_copy(buf, ss, rs, at(off) * CORES + other).start()
        for off in (2, -2):
            bias_copy(buf, ss, rs, at(off) * CORES + core).start()

    def bias_wait(buf, ss, rs, src):
        remote(buf.at[src], buf.at[src], ss, rs.at[src], partner).wait_recv()

    def forward(buf, ss, rs, c):
        src = c * CORES + core
        return remote(buf.at[src], buf.at[src], ss, rs.at[src], partner)

    def fetch(buf, ss, rs, c):
        bias_wait(buf, ss, rs, c * CORES + core)
        forward(buf, ss, rs, c).start()

    def relay(buf, ss, rs):
        for sign in (1, -1):
            origin = at(-2 * sign) * CORES + core
            bias_wait(buf, ss, rs, origin)
            row = buf.at[origin]
            remote(row, row, ss, rs.at[origin], at(sign) * CORES + core).start()

            @pl.when(core == (1 - sign) // 2)
            def _():
                remote(row, row, ss, rs.at[origin], at(2 * sign) * CORES + core).start()
            forward(buf, ss, rs, at(-2 * sign)).start()

    def sent(buf, ss, rs):
        remote(buf, buf, ss, rs, partner).wait_send()

    def put_u(r, u):
        u_s[r] = u

    w_loads[0].wait()
    with jax.named_scope("bias_rows"):
        pair_bias(lambda i: z_load(i).wait(), lambda r: z_ref[r], put_u, wb_s, brecv)
    with jax.named_scope("barrier"):
        pl.semaphore_wait(barrier, len(greeted))
    bias_send(brecv, b_ss, b_rs, True)
    for cp in w_loads[1:]:
        cp.wait()


    def project(i, carry):
        rs = [PROJ_UNROLL * i + t for t in range(PROJ_UNROLL)]
        prs = [mm(u_s[r], wp_s[...]) for r in rs]
        for r, pr in zip(rs, prs):
            q_s[r] = pr[:, :chan].astype(BF16)
            kt_s[r] = pr[:, chan:2 * chan].T.astype(BF16)
            v_s[r] = pr[:, 2 * chan:3 * chan].astype(BF16)
            g_s[r] = sigmoid(pr[:, 3 * chan:])
        return carry

    with jax.named_scope("project"):
        lax.fori_loop(0, rows // PROJ_UNROLL, project, 0)

    def attention(qs, kts, vs, biases, gates, wo):
        nrow = qs[0].shape[0]
        qm = [jnp.concatenate([jnp.where(lane_head == h, q, jnp.zeros_like(q)) for h in range(heads)], axis=0) for q in qs]
        sc = [mm(a, kt) * scale + b[...] for a, kt, b in zip(qm, kts, biases)]
        pe = [jnp.exp(s - jnp.max(s, axis=-1, keepdims=True)) for s in sc]
        ls = [1.0 / jnp.sum(e, axis=-1, keepdims=True) for e in pe]
        os = [mm(e.astype(BF16), v) * l for e, v, l in zip(pe, vs, ls)]
        upds = []
        for o, gate in zip(os, gates):
            mix = sum(jnp.where(lane_head == h, o[h * nrow:(h + 1) * nrow], 0.0) for h in range(heads))
            upds.append(mm((mix * gate).astype(BF16), wo[...]))
        return upds

    def h_copy(dev, hf):
        return remote(hsend.at[pl.ds(dev * rows + hf * part, part)],
                      ht.at[pl.ds(hf * part, part), pl.ds(aligned(me * rows, rows), rows), :], h_ss, h_rs.at[hf], dev)

    wide = CORES * rows

    def start_block(cs, between):
        nc = len(cs)
        nq = nc * wide
        for h in range(heads):
            for k in range(nc * CORES):
                src = brecv[cs[k // CORES] * CORES + k % CORES, h * rows:(h + 1) * rows, :]
                bias_f[h * nq + k * rows:h * nq + (k + 1) * rows, :] = src.astype(F32)
        cols = [pl.ds(aligned(c * wide, wide), wide) for c in cs]
        bias = bias_f.at[pl.ds(0, heads * nq)]

        def attend(i, carry):
            rs = [ROW_UNROLL * i + t for t in range(ROW_UNROLL)]
            qs = [jnp.concatenate([q_s[r, sl, :] for sl in cols], axis=0) for r in rs]
            gates = [jnp.concatenate([g_s[r, sl, :] for sl in cols], axis=0) for r in rs]
            upds = attention(qs, [kt_s[r] for r in rs], [v_s[r] for r in rs], [bias] * len(rs), gates, wo_s)
            for r, upd in zip(rs, upds):
                z1 = jnp.concatenate([z_ref[r, sl, :] for sl in cols], axis=0) + upd
                for k, c in enumerate(cs):
                    z1_ref[pl.ds(aligned(r * seq + c * wide, wide), wide), :] = z1[k * wide:(k + 1) * wide]
                zb[pl.ds(aligned(r * (nq + PAD), PAD), nq), :] = z1
            return carry

        half = rows // ROW_UNROLL // 2
        with jax.named_scope("attend_a"):
            lax.fori_loop(0, half, attend, 0)
        with jax.named_scope("fetch_next"):
            between()
        with jax.named_scope("attend_b"):
            lax.fori_loop(half, 2 * half, attend, 0)
        for k, c in enumerate(cs):
            for j in range(wide):
                hsend[c * wide + j] = zb[pl.ds(k * wide + j, rows, stride=nq + PAD), :].astype(BF16)

    def wait_other(c):
        with jax.named_scope("wait_block"):
            bias_wait(brecv, b_ss, b_rs, c * CORES + other)

    def fetch_ring(dist):
        fetch(brecv, b_ss, b_rs, at(dist))

        @pl.when(2 * dist < chips)
        def _():
            fetch(brecv, b_ss, b_rs, at(-dist))

    def send_ring(cs, hf):
        for s in range(CORES):
            for c in cs:
                h_copy(c * CORES + s, hf).start()

    bias_wait(brecv, b_ss, b_rs, partner)
    start_block([chip], lambda: None)
    for off in (1, -1):
        bias_wait(brecv, b_ss, b_rs, at(off) * CORES + core)
    for hf in range(HALVES):
        h_copy(partner, hf).start()

    def start_ring(dist, carry):
        cs = [at(dist), at(-dist)]
        for c in cs:
            wait_other(c)
        def between():
            @pl.when(dist == 1)
            def _():
                relay(brecv, b_ss, b_rs)

            @pl.when(dist > 1)
            def _():
                fetch_ring(dist + 1)

        start_block(cs, between)
        send_ring(cs, 0)
        for hf in range(1, HALVES):
            @pl.when(dist < HOLD_FROM)
            def _():
                send_ring(cs, hf)
        return carry

    far = chips // 2
    lax.fori_loop(1, far, start_ring, 0)
    wait_other(at(far))
    start_block([at(far)], lambda: None)

    with jax.named_scope("bias_cols"):
        pair_bias(lambda i: None, lambda r: z1_ref[pl.ds(aligned(r * seq, seq), seq), :].astype(BF16).astype(F32), None, wb_e, erecv)
    bias_send(erecv, e_ss, e_rs, False)
    send_ring([at(far)], 0)
    ht[:, pl.ds(aligned(me * rows, rows), rows), :] = hsend[pl.ds(aligned(me * rows, rows), rows)]

    with jax.named_scope("wait_cols"):
        relay(erecv, e_ss, e_rs)
        for hf in range(1, HALVES):
            for dist in range(HOLD_FROM, far):
                send_ring([at(dist), at(-dist)], hf)
            send_ring([at(far)], hf)
        for off in (1, -1, 3, -3, 4):
            fetch(erecv, e_ss, e_rs, at(off))
        for c in range(chips):
            bias_wait(erecv, e_ss, e_rs, c * CORES + other)

    def widen(h, carry):
        tall = jnp.concatenate([erecv[dev, pl.ds(aligned(h * rows, rows), rows), :] for dev in range(n)], axis=0)
        bias_e[pl.ds(aligned(h * seq, seq), seq), :] = tall.astype(F32).T
        return carry

    with jax.named_scope("widen"):
        lax.fori_loop(0, heads, widen, 0)

    def is_far(off):
        return int(min(off // CORES, chips - off // CORES) > 2)

    def d_copy(off, grp):
        dev = lax.rem(me // CORES * CORES + off // CORES * CORES, n) + (core if off % CORES == 0 else other)
        return remote(dsend.at[pl.ds(grp * COL_GROUP, COL_GROUP), pl.ds(aligned(dev * rows, rows), rows), :],
                      drecv.at[pl.ds(me * rows + grp * COL_GROUP, COL_GROUP)],
                      d_ss, d_rs.at[grp // (part // COL_GROUP), is_far(off)], dev)

    def end_cols(i, carry):
        js = [COL_UNROLL * i + t for t in range(COL_UNROLL)]
        hs = [ht[j] for j in js]
        us = [norm(h.astype(F32)) for h in hs]
        prs = [mm(u, wp_e[...]) for u in us]
        kts = [p[:, chan:2 * chan].T.astype(BF16) for p in prs]
        es = attention([p[:, :chan].astype(BF16) for p in prs], kts, [p[:, 2 * chan:3 * chan].astype(BF16) for p in prs],
                       [bias_e] * len(js), [sigmoid(p[:, 3 * chan:]) for p in prs], wo_e)
        z2 = [h.astype(F32) + e for h, e in zip(hs, es)]
        hid = [jnp.maximum(mm(norm(z), w1[...]), 0.0).astype(BF16) for z in z2]
        ts = [mm(x, w2[...]) for x in hid]
        for j, e, t in zip(js, es, ts):
            dsend[j] = (e + t).astype(BF16)
        return carry

    far_first = sorted(range(1, n), key=lambda off: -min(off // CORES, chips - off // CORES))
    per = COL_GROUP // COL_UNROLL

    def end_group(grp, carry):
        for hf in range(HALVES):
            @pl.when(grp == hf * (part // COL_GROUP))
            def _():
                with jax.named_scope("wait_h"):
                    whole = hsend.at[pl.ds(0, (n - 1) * part)]
                    remote(whole, whole, h_ss, h_rs.at[hf], partner).wait_recv()
        with jax.named_scope("end_cols"):
            lax.fori_loop(grp * per, (grp + 1) * per, end_cols, 0)
        for off in far_first:
            d_copy(off, grp).start()
        return carry

    lax.fori_loop(0, rows // COL_GROUP, end_group, 0)
    drecv[pl.ds(me * rows, rows)] = dsend[:, pl.ds(aligned(me * rows, rows), rows), :]

    pitch = rows + PAD
    with jax.named_scope("finish"):
        for hf in range(HALVES):
            def finish(first, k, carry):
                dev = at(first + k // CORES) * CORES + lax.rem(k, CORES)
                base = dev * (part * pitch)
                for t in range(part):
                    tmp[pl.ds(aligned(base + t * pitch, PAD), rows), :] = drecv[dev * rows + hf * part + t].astype(F32)
                for i in range(rows):
                    z1_ref[pl.ds(aligned(i * seq + dev * rows + hf * part, part), part), :] += tmp[pl.ds(base + i, part, stride=pitch), :]
                return carry

            for side, first, num in ((0, -2, 5), (1, 3, chips - 5)):
                arrived = drecv.at[pl.ds(0, (num * CORES - (1 - side)) * part)]
                remote(arrived, arrived, d_ss, d_rs.at[hf, side], partner).wait_recv()
                lax.fori_loop(0, num * CORES, functools.partial(finish, first), 0)

    with jax.named_scope("drain"):
        for buf, ss, rs in ((brecv, b_ss, b_rs), (erecv, e_ss, e_rs)):
            sent(buf.at[pl.ds(0, n - 1)], ss, rs.at[0])
        sent(hsend.at[pl.ds(0, (n - 1) * rows)], h_ss, h_rs.at[0])
        sent(dsend.at[pl.ds(0, n - 1)], d_ss, d_rs.at[0, 0])


def solution(mesh):
    row_spec = P(('dp', AXIS), None, None)
    n = mesh.shape[AXIS]

    def local_fn(z, *weights):
        rows, seq, chan = z.shape
        heads = weights[1].shape[0]
        hrows = heads * rows
        part = rows // HALVES
        nq = 2 * CORES * rows
        dma = pltpu.SemaphoreType.DMA
        vmem = pl.BlockSpec(memory_space=pltpu.VMEM)
        y = pl.pallas_call(
            functools.partial(kernel, n, rows, seq, heads),
            out_shape=jax.ShapeDtypeStruct((rows * seq, chan), F32),
            in_specs=[pl.BlockSpec(memory_space=pltpu.HBM)] * 9,
            out_specs=vmem,
            scratch_shapes=[pltpu.VMEM(z.shape, z.dtype)] + [pltpu.VMEM(w.shape, w.dtype) for w in weights] + [
                pltpu.VMEM((rows, seq, chan), BF16),
                pltpu.VMEM((rows, seq, chan), BF16),
                pltpu.VMEM((rows, chan, seq), BF16),
                pltpu.VMEM((rows, seq, chan), BF16),
                pltpu.VMEM((rows, seq, chan), F32),
                pltpu.VMEM((LN_ROWS, seq, chan), F32), pltpu.VMEM((LN_ROWS, seq, chan), F32),
                pltpu.VMEM((n, hrows, seq), BF16),
                pltpu.VMEM((heads * nq, seq), F32),
                pltpu.VMEM((rows * (nq + PAD), chan), F32),
                pltpu.VMEM((seq, rows, chan), BF16),
                pltpu.VMEM((rows, seq, chan), BF16),
                pltpu.VMEM((n, hrows, seq), BF16),
                pltpu.VMEM((heads * seq, seq), F32),
                pltpu.VMEM((rows, seq, chan), BF16),
                pltpu.VMEM((seq, rows, chan), BF16),
                pltpu.VMEM((n * part * (rows + PAD), chan), F32),
                dma((rows // LN_ROWS,)), dma((len(weights),)),
                dma, dma((n,)), dma, dma((n,)), dma, dma((HALVES,)), dma, dma((HALVES, 2)),
            ],
            compiler_params=pltpu.CompilerParams(collective_id=0, has_side_effects=True, vmem_limit_bytes=40 * 2 ** 20),
        )(*[pltpu.with_memory_space_constraint(a, pltpu.HBM) for a in (z,) + weights])
        return y.reshape(rows, seq, chan)

    return jax.shard_map(local_fn, mesh=mesh, in_specs=(row_spec,) + (P(),) * 8, out_specs=row_spec, check_vma=False)
```

```python
import functools

import jax
import jax.numpy as jnp
from jax import lax
from jax.experimental import pallas as pl
from jax.experimental.pallas import tpu as pltpu
from jax.sharding import PartitionSpec as P

LN_EPS = 1e-5
F32, BF16 = jnp.float32, jnp.bfloat16
MESH = pl.DeviceIdType.MESH
AXIS = "sp"
CORES = 2
HALVES = 2
COL_GROUP = 2
HOLD_FROM = 2
ROW_UNROLL = 8
COL_UNROLL = 2
LN_ROWS = 4
PROJ_UNROLL = 8
PAD = 8


def norm(vals):
    mean_c = jnp.mean(vals, axis=-1, keepdims=True)
    centered = vals - mean_c
    variance = jnp.mean(centered * centered, axis=-1, keepdims=True)
    return (centered * lax.rsqrt(variance + LN_EPS)).astype(BF16)


def mm(a, b, ca=1, cb=0):
    return lax.dot_general(a, b, (((ca,), (cb,)), ((), ())), preferred_element_type=F32)


def sigmoid(x):
    return 1.0 / (1.0 + jnp.exp(-x))


def kernel(n, rows, seq, heads, z_hbm, wps_h, wbs_h, wos_h, wpe_h, wbe_h, woe_h, w1_h, w2_h,
           z1_ref,
           z_ref, wp_s, wb_s, wo_s, wp_e, wb_e, wo_e, w1, w2,
           u_s, q_s, kt_s, v_s, g_s, cen_a, cen_b, brecv, bias_f, zb, hsend, ht, erecv, bias_e, dsend, drecv, tmp,
           z_sem, w_sem, b_ss, b_rs, e_ss, e_rs, h_ss, h_rs, d_ss, d_rs):
    cen = (cen_a, cen_b)
    chan = wo_s.shape[0]
    hd = chan // heads
    scale = hd ** -0.5
    chips = n // CORES
    part = rows // HALVES
    me = lax.axis_index(AXIS)
    chip, core = me // CORES, lax.rem(me, CORES)
    other = CORES - 1 - core
    partner = chip * CORES + other
    hrows = heads * rows

    def remote(src, dst, ss, rs, dev):
        return pltpu.make_async_remote_copy(src_ref=src, dst_ref=dst, send_sem=ss, recv_sem=rs,
                                            device_id={AXIS: dev}, device_id_type=MESH)

    def aligned(i, k):
        return pl.multiple_of(i, k)

    def z_load(i):
        sl = pl.ds(i * LN_ROWS, LN_ROWS)
        return pltpu.make_async_copy(z_hbm.at[sl], z_ref.at[sl], z_sem.at[i])

    def z_row(r):
        return pltpu.make_async_copy(z_hbm.at[r], z_ref.at[r], z_sem.at[r // LN_ROWS])

    w_loads = [pltpu.make_async_copy(src, dst, w_sem.at[i]) for i, (src, dst) in enumerate(
        [(wbs_h, wb_s), (wps_h, wp_s), (wos_h, wo_s), (wbe_h, wb_e), (wpe_h, wp_e), (woe_h, wo_e), (w1_h, w1), (w2_h, w2)])]
    w_loads[0].start()
    for r in range(rows):
        z_row(r).start()
    for cp in w_loads[1:]:
        cp.start()

    barrier = pltpu.get_barrier_semaphore()
    greeted = [partner] + [lax.rem(chip + off + chips, chips) * CORES + s for off in (1, -1, 2, -2) for s in range(CORES)]
    for dev in greeted:
        pl.semaphore_signal(barrier, 1, device_id={AXIS: dev}, device_id_type=MESH)

    row_of = lax.rem(lax.broadcasted_iota(jnp.int32, (hrows, chan), 0), rows)
    lane_head = lax.broadcasted_iota(jnp.int32, (1, chan), 1) // hd

    def pair_bias(ready, get_row, put_row, wb, out):
        wide = wb[...].astype(F32)
        wide = jnp.concatenate([jnp.broadcast_to(wide[h:h + 1], (rows, chan)) for h in range(heads)], axis=0)
        total = jnp.zeros((hrows, seq), F32)
        steps = rows // LN_ROWS
        for i in range(steps + 1):
            if i < steps:
                ready(i)
                for t in range(LN_ROWS):
                    vals = get_row(i * LN_ROWS + t)
                    cen[i % 2][t] = vals - jnp.mean(vals, axis=-1, keepdims=True)
            if i:
                for t in range(LN_ROWS):
                    r = (i - 1) * LN_ROWS + t
                    centered = cen[(i - 1) % 2][t]
                    variance = jnp.mean(centered * centered, axis=-1, keepdims=True)
                    u = (centered * lax.rsqrt(variance + LN_EPS)).astype(BF16)
                    if put_row is not None:
                        put_row(r, u)
                    total += mm(jnp.where(row_of == r, wide, 0.0).astype(BF16), u, 1, 1)
        out[me] = total.astype(BF16)

    def bias_copy(buf, ss, rs, dev):
        return remote(buf.at[me], buf.at[me], ss, rs.at[me], dev)

    def at(off):
        return lax.rem(chip + off + chips, chips)

    def bias_send(buf, ss, rs, both):
        bias_copy(buf, ss, rs, partner).start()
        for off in (1, -1):
            bias_copy(buf, ss, rs, at(off) * CORES + core).start()
        for off in (1, -1) if both else ():
            bias_copy(buf, ss, rs, at(off) * CORES + other).start()
        for off in (2, -2):
            bias_copy(buf, ss, rs, at(off) * CORES + core).start()

    def bias_wait(buf, ss, rs, src):
        remote(buf.at[src], buf.at[src], ss, rs.at[src], partner).wait_recv()

    def forward(buf, ss, rs, c):
        src = c * CORES + core
        return remote(buf.at[src], buf.at[src], ss, rs.at[src], partner)

    def fetch(buf, ss, rs, c):
        bias_wait(buf, ss, rs, c * CORES + core)
        forward(buf, ss, rs, c).start()

    def relay(buf, ss, rs):
        for sign in (1, -1):
            origin = at(-2 * sign) * CORES + core
            bias_wait(buf, ss, rs, origin)
            row = buf.at[origin]
            remote(row, row, ss, rs.at[origin], at(sign) * CORES + core).start()

            @pl.when(core == (1 - sign) // 2)
            def _():
                remote(row, row, ss, rs.at[origin], at(2 * sign) * CORES + core).start()
            forward(buf, ss, rs, at(-2 * sign)).start()

    def sent(buf, ss, rs):
        remote(buf, buf, ss, rs, partner).wait_send()

    def put_u(r, u):
        u_s[r] = u

    w_loads[0].wait()
    with jax.named_scope("bias_rows"):
        pair_bias(lambda i: z_load(i).wait(), lambda r: z_ref[r], put_u, wb_s, brecv)
    with jax.named_scope("barrier"):
        pl.semaphore_wait(barrier, len(greeted))
    bias_send(brecv, b_ss, b_rs, True)
    for cp in w_loads[1:]:
        cp.wait()


    def project(i, carry):
        rs = [PROJ_UNROLL * i + t for t in range(PROJ_UNROLL)]
        prs = [mm(u_s[r], wp_s[...]) for r in rs]
        for r, pr in zip(rs, prs):
            q_s[r] = pr[:, :chan].astype(BF16)
            kt_s[r] = pr[:, chan:2 * chan].T.astype(BF16)
            v_s[r] = pr[:, 2 * chan:3 * chan].astype(BF16)
            g_s[r] = sigmoid(pr[:, 3 * chan:])
        return carry

    with jax.named_scope("project"):
        lax.fori_loop(0, rows // PROJ_UNROLL, project, 0)

    def attention(qs, kts, vs, biases, gates, wo):
        nrow = qs[0].shape[0]
        qm = [jnp.concatenate([jnp.where(lane_head == h, q, jnp.zeros_like(q)) for h in range(heads)], axis=0) for q in qs]
        sc = [mm(a, kt) * scale + b[...] for a, kt, b in zip(qm, kts, biases)]
        pe = [jnp.exp(s - jnp.max(s, axis=-1, keepdims=True)) for s in sc]
        ls = [1.0 / jnp.sum(e, axis=-1, keepdims=True) for e in pe]
        os = [mm(e.astype(BF16), v) * l for e, v, l in zip(pe, vs, ls)]
        upds = []
        for o, gate in zip(os, gates):
            mix = sum(jnp.where(lane_head == h, o[h * nrow:(h + 1) * nrow], 0.0) for h in range(heads))
            upds.append(mm((mix * gate).astype(BF16), wo[...]))
        return upds

    def h_copy(dev, hf):
        return remote(hsend.at[pl.ds(dev * rows + hf * part, part)],
                      ht.at[pl.ds(hf * part, part), pl.ds(aligned(me * rows, rows), rows), :], h_ss, h_rs.at[hf], dev)

    wide = CORES * rows

    def start_block(cs, between):
        nc = len(cs)
        nq = nc * wide
        for h in range(heads):
            for k in range(nc * CORES):
                src = brecv[cs[k // CORES] * CORES + k % CORES, h * rows:(h + 1) * rows, :]
                bias_f[h * nq + k * rows:h * nq + (k + 1) * rows, :] = src.astype(F32)
        cols = [pl.ds(aligned(c * wide, wide), wide) for c in cs]
        bias = bias_f.at[pl.ds(0, heads * nq)]

        def attend(i, carry):
            rs = [ROW_UNROLL * i + t for t in range(ROW_UNROLL)]
            qs = [jnp.concatenate([q_s[r, sl, :] for sl in cols], axis=0) for r in rs]
            gates = [jnp.concatenate([g_s[r, sl, :] for sl in cols], axis=0) for r in rs]
            upds = attention(qs, [kt_s[r] for r in rs], [v_s[r] for r in rs], [bias] * len(rs), gates, wo_s)
            for r, upd in zip(rs, upds):
                z1 = jnp.concatenate([z_ref[r, sl, :] for sl in cols], axis=0) + upd
                for k, c in enumerate(cs):
                    z1_ref[pl.ds(aligned(r * seq + c * wide, wide), wide), :] = z1[k * wide:(k + 1) * wide]
                zb[pl.ds(aligned(r * (nq + PAD), PAD), nq), :] = z1
            return carry

        half = rows // ROW_UNROLL // 2
        with jax.named_scope("attend_a"):
            lax.fori_loop(0, half, attend, 0)
        with jax.named_scope("fetch_next"):
            between()
        with jax.named_scope("attend_b"):
            lax.fori_loop(half, 2 * half, attend, 0)
        for k, c in enumerate(cs):
            for j in range(wide):
                hsend[c * wide + j] = zb[pl.ds(k * wide + j, rows, stride=nq + PAD), :].astype(BF16)

    def wait_other(c):
        with jax.named_scope("wait_block"):
            bias_wait(brecv, b_ss, b_rs, c * CORES + other)

    def fetch_ring(dist):
        fetch(brecv, b_ss, b_rs, at(dist))

        @pl.when(2 * dist < chips)
        def _():
            fetch(brecv, b_ss, b_rs, at(-dist))

    def send_ring(cs, hf):
        for s in range(CORES):
            for c in cs:
                h_copy(c * CORES + s, hf).start()

    bias_wait(brecv, b_ss, b_rs, partner)
    start_block([chip], lambda: None)
    for off in (1, -1):
        bias_wait(brecv, b_ss, b_rs, at(off) * CORES + core)
    for hf in range(HALVES):
        h_copy(partner, hf).start()

    def start_ring(dist, carry):
        cs = [at(dist), at(-dist)]
        for c in cs:
            wait_other(c)
        def between():
            @pl.when(dist == 1)
            def _():
                relay(brecv, b_ss, b_rs)

            @pl.when(dist > 1)
            def _():
                fetch_ring(dist + 1)

        start_block(cs, between)
        send_ring(cs, 0)
        for hf in range(1, HALVES):
            @pl.when(dist < HOLD_FROM)
            def _():
                send_ring(cs, hf)
        return carry

    far = chips // 2
    lax.fori_loop(1, far, start_ring, 0)
    wait_other(at(far))
    start_block([at(far)], lambda: None)

    with jax.named_scope("bias_cols"):
        pair_bias(lambda i: None, lambda r: z1_ref[pl.ds(aligned(r * seq, seq), seq), :].astype(BF16).astype(F32), None, wb_e, erecv)
    bias_send(erecv, e_ss, e_rs, False)
    send_ring([at(far)], 0)
    ht[:, pl.ds(aligned(me * rows, rows), rows), :] = hsend[pl.ds(aligned(me * rows, rows), rows)]

    with jax.named_scope("wait_cols"):
        relay(erecv, e_ss, e_rs)
        for hf in range(1, HALVES):
            for dist in range(HOLD_FROM, far):
                send_ring([at(dist), at(-dist)], hf)
            send_ring([at(far)], hf)
        for off in (1, -1, 3, -3, 4):
            fetch(erecv, e_ss, e_rs, at(off))
        for c in range(chips):
            bias_wait(erecv, e_ss, e_rs, c * CORES + other)

    def widen(h, carry):
        tall = jnp.concatenate([erecv[dev, pl.ds(aligned(h * rows, rows), rows), :] for dev in range(n)], axis=0)
        bias_e[pl.ds(aligned(h * seq, seq), seq), :] = tall.astype(F32).T
        return carry

    with jax.named_scope("widen"):
        lax.fori_loop(0, heads, widen, 0)

    def ring_dist(off):
        return min(off // CORES, chips - off // CORES)

    def d_copy(off, first, count, hf):
        dev = lax.rem(me // CORES * CORES + off // CORES * CORES, n) + (core if off % CORES == 0 else other)
        return remote(dsend.at[pl.ds(first, count), pl.ds(aligned(dev * rows, rows), rows), :],
                      drecv.at[pl.ds(me * rows + first, count)], d_ss, d_rs.at[hf, int(ring_dist(off) > 2)], dev)

    def end_cols(i, carry):
        js = [COL_UNROLL * i + t for t in range(COL_UNROLL)]
        hs = [ht[j] for j in js]
        us = [norm(h.astype(F32)) for h in hs]
        prs = [mm(u, wp_e[...]) for u in us]
        kts = [p[:, chan:2 * chan].T.astype(BF16) for p in prs]
        es = attention([p[:, :chan].astype(BF16) for p in prs], kts, [p[:, 2 * chan:3 * chan].astype(BF16) for p in prs],
                       [bias_e] * len(js), [sigmoid(p[:, 3 * chan:]) for p in prs], wo_e)
        z2 = [h.astype(F32) + e for h, e in zip(hs, es)]
        hid = [jnp.maximum(mm(norm(z), w1[...]), 0.0).astype(BF16) for z in z2]
        ts = [mm(x, w2[...]) for x in hid]
        for j, e, t in zip(js, es, ts):
            dsend[j] = (e + t).astype(BF16)
        return carry

    far_first = sorted(range(1, n), key=lambda off: -ring_dist(off))
    per = COL_GROUP // COL_UNROLL

    def end_group(grp, carry):
        for hf in range(HALVES):
            @pl.when(grp == hf * (part // COL_GROUP))
            def _():
                with jax.named_scope("wait_h"):
                    whole = hsend.at[pl.ds(0, (n - 1) * part)]
                    remote(whole, whole, h_ss, h_rs.at[hf], partner).wait_recv()
        with jax.named_scope("end_cols"):
            lax.fori_loop(grp * per, (grp + 1) * per, end_cols, 0)
        for off in far_first:
            if ring_dist(off) != 1:
                d_copy(off, grp * COL_GROUP, COL_GROUP, grp // (part // COL_GROUP)).start()
        return carry

    lax.fori_loop(0, rows // COL_GROUP, end_group, 0)
    for hf in range(HALVES):
        for off in far_first:
            if ring_dist(off) == 1:
                d_copy(off, hf * part, part, hf).start()
    drecv[pl.ds(me * rows, rows)] = dsend[:, pl.ds(aligned(me * rows, rows), rows), :]

    pitch = rows + PAD
    with jax.named_scope("finish"):
        for hf in range(HALVES):
            def finish(first, k, carry):
                dev = at(first + k // CORES) * CORES + lax.rem(k, CORES)
                base = dev * (part * pitch)
                for t in range(part):
                    tmp[pl.ds(aligned(base + t * pitch, PAD), rows), :] = drecv[dev * rows + hf * part + t].astype(F32)
                for i in range(rows):
                    z1_ref[pl.ds(aligned(i * seq + dev * rows + hf * part, part), part), :] += tmp[pl.ds(base + i, part, stride=pitch), :]
                return carry

            for side, first, num in ((0, -2, 5), (1, 3, chips - 5)):
                arrived = drecv.at[pl.ds(0, (num * CORES - (1 - side)) * part)]
                remote(arrived, arrived, d_ss, d_rs.at[hf, side], partner).wait_recv()
                lax.fori_loop(0, num * CORES, functools.partial(finish, first), 0)

    with jax.named_scope("drain"):
        for buf, ss, rs in ((brecv, b_ss, b_rs), (erecv, e_ss, e_rs)):
            sent(buf.at[pl.ds(0, n - 1)], ss, rs.at[0])
        sent(hsend.at[pl.ds(0, (n - 1) * rows)], h_ss, h_rs.at[0])
        sent(dsend.at[pl.ds(0, n - 1)], d_ss, d_rs.at[0, 0])


def solution(mesh):
    row_spec = P(('dp', AXIS), None, None)
    n = mesh.shape[AXIS]

    def local_fn(z, *weights):
        rows, seq, chan = z.shape
        heads = weights[1].shape[0]
        hrows = heads * rows
        part = rows // HALVES
        nq = 2 * CORES * rows
        dma = pltpu.SemaphoreType.DMA
        vmem = pl.BlockSpec(memory_space=pltpu.VMEM)
        y = pl.pallas_call(
            functools.partial(kernel, n, rows, seq, heads),
            out_shape=jax.ShapeDtypeStruct((rows * seq, chan), F32),
            in_specs=[pl.BlockSpec(memory_space=pltpu.HBM)] * 9,
            out_specs=vmem,
            scratch_shapes=[pltpu.VMEM(z.shape, z.dtype)] + [pltpu.VMEM(w.shape, w.dtype) for w in weights] + [
                pltpu.VMEM((rows, seq, chan), BF16),
                pltpu.VMEM((rows, seq, chan), BF16),
                pltpu.VMEM((rows, chan, seq), BF16),
                pltpu.VMEM((rows, seq, chan), BF16),
                pltpu.VMEM((rows, seq, chan), F32),
                pltpu.VMEM((LN_ROWS, seq, chan), F32), pltpu.VMEM((LN_ROWS, seq, chan), F32),
                pltpu.VMEM((n, hrows, seq), BF16),
                pltpu.VMEM((heads * nq, seq), F32),
                pltpu.VMEM((rows * (nq + PAD), chan), F32),
                pltpu.VMEM((seq, rows, chan), BF16),
                pltpu.VMEM((rows, seq, chan), BF16),
                pltpu.VMEM((n, hrows, seq), BF16),
                pltpu.VMEM((heads * seq, seq), F32),
                pltpu.VMEM((rows, seq, chan), BF16),
                pltpu.VMEM((seq, rows, chan), BF16),
                pltpu.VMEM((n * part * (rows + PAD), chan), F32),
                dma((rows // LN_ROWS,)), dma((len(weights),)),
                dma, dma((n,)), dma, dma((n,)), dma, dma((HALVES,)), dma, dma((HALVES, 2)),
            ],
            compiler_params=pltpu.CompilerParams(collective_id=0, has_side_effects=True, vmem_limit_bytes=40 * 2 ** 20),
        )(*[pltpu.with_memory_space_constraint(a, pltpu.HBM) for a in (z,) + weights])
        return y.reshape(rows, seq, chan)

    return jax.shard_map(local_fn, mesh=mesh, in_specs=(row_spec,) + (P(),) * 8, out_specs=row_spec, check_vma=False)
```
